32 devices in a mesh: dp: 4 (over y, x), mp: 8 (over z, core).
Axes of the slice: x: 2, y: 2, z: 4, core: 2. Of those that a mesh axis runs over, the one named last changes fastest.
Arguments:
- data_rows: bfloat16 [16384, 2048], P(('dp', 'mp')), may hold values from -32 to 32
- centroids: bfloat16 [12288, 2048], P('mp'), may hold values from -0.75 to 0.75
- block_mask: int32 [8, 128], P(None, ('dp', 'mp')), may hold values from 0 to 1, as said below
- lower_bound: float32 [8, 16384], P(None, ('dp', 'mp')), may hold values from 0 to 4
Outputs:
- new_centroids: float32 [12288, 2048], P(('mp', 'dp'))
- centroid_shift: float32 [12288], P(('mp', 'dp'))
- log_norm: float32 [16384], P(('dp', 'mp'))
- new_lower: float32 [8, 16384], P(None, ('dp', 'mp'))
The draws below stay inside these ranges and needn't reach their ends.
Inputs may be any that keep to these rules, and one draw needn't show every extreme that they name: `block_mask`: within the 4 blocks of one device (aligned runs along the last dimension), at most 1 are 1 for each shard; for some shard every device has exactly 1.
All inputs are finite; a program needn't handle non-finite values.
Results may differ from the reference program's by a relative error of at most 0.0011.
Values may be sent and summed in bfloat16 or wider, within the bound.
No kernel may reach another device: no remote copies, remote signals or barrier semaphores. Data moves between devices by JAX's collectives and lax.ppermute only.
A program may use at most 128 MiB of HBM per device.

```python
import math
import jax
import jax.numpy as jnp
from jax import lax

F = 2048
K = 12288
BLOCK = 128
SLOTS = 1
ROW_DEV = 512
ROWS = 16384
NBLOCKS = 128
N_MP = 8


def draw_masks(key):
    device_count = ROWS // ROW_DEV
    block_count = ROW_DEV // BLOCK
    base = jax.random.fold_in(key, 11)
    key_bits, key_heavy, key_forced, key_count = jax.random.split(base, 4)
    bits = jax.random.randint(key_bits, (device_count, N_MP, block_count), 0, 1 << 20)
    distinct = bits * block_count + jnp.arange(block_count, dtype=jnp.int32)[None, None, :]
    order = jnp.argsort(distinct, axis=-1)
    block_rank = jnp.argsort(order, axis=-1)
    heavy = jax.random.randint(key_heavy, (N_MP,), 0, 4) == 0
    forced = jax.random.randint(key_forced, (), 0, N_MP)
    heavy = heavy | (jnp.arange(N_MP) == forced)
    chosen_count = jax.random.randint(key_count, (device_count, N_MP), 0, SLOTS + 1)
    chosen_count = jnp.where(heavy[None, :], SLOTS, chosen_count)
    active = (block_rank < chosen_count[:, :, None]).astype(jnp.int32)
    return active.transpose(1, 0, 2).reshape(N_MP, NBLOCKS)


def draw_cents(key):
    base = jax.random.fold_in(key, 23)
    values = 0.125 * jax.random.normal(base, (K, F), jnp.float32)
    return jnp.clip(values, -0.75, 0.75)


def draw_block_mask(key, part):
    return draw_masks(key)


def draw_centroids(key, part):
    return draw_cents(key).astype(jnp.bfloat16)


def draw_data_rows(key, part):
    base = jax.random.fold_in(key, 37)
    key_main = jax.random.fold_in(base, 0)
    values = jnp.clip(jax.random.normal(key_main, (ROWS, F), jnp.float32), -6.0, 6.0)
    return values.astype(jnp.bfloat16)


def steps_of(rng, extent, shards, low, largest):
    def one(axis_at, blocks):
        draws = jax.random.uniform(jax.random.fold_in(jax.random.fold_in(rng, 6), axis_at), (blocks,), jnp.float32, low / len(shards), largest / len(shards))
        return jnp.repeat(jnp.exp(draws), extent[axis_at] // blocks).reshape((-1,) + (1,) * (len(extent) - axis_at - 1))

    level = one(*shards[0])
    for cut in shards[1:]:
        level = level * one(*cut)
    return level


def setup_inputs(seed: int = 0) -> dict:
    key_of = jax.random.split(jax.random.key(seed), 5)
    return {
        "data_rows": draw_data_rows(jax.random.fold_in(key_of[4], 71), 0),
        "centroids": draw_centroids(jax.random.fold_in(key_of[4], 71), 0),
        "block_mask": draw_block_mask(jax.random.fold_in(key_of[4], 71), 0),
        "lower_bound": jnp.clip(4.0 * jax.random.uniform(key_of[3], (N_MP, ROWS), jnp.float32) ** steps_of(key_of[3], (N_MP, ROWS), ((1, 32),), -0.2, 0.2), 0.0, 4.0),
    }


def pack_codes(mask_dev):
    block_count = mask_dev.shape[1]
    block_rank = (jnp.cumsum(mask_dev, axis=1) - 1).astype(jnp.int32)
    slot_ids = jnp.arange(SLOTS, dtype=jnp.int32)
    chosen = (mask_dev[:, None, :] == 1) & (block_rank[:, None, :] == slot_ids[None, :, None])
    labels = jnp.arange(1, block_count + 1, dtype=jnp.int32)
    return lax.optimization_barrier(jnp.sum(jnp.where(chosen, labels[None, None, :], 0), axis=2)).astype(jnp.int32)

def combine_rows(slot_codes, row_top, row_mass, block_count):
    labels = jnp.arange(1, block_count + 1, dtype=jnp.int32)
    is_slot = slot_codes[:, :, None] == labels[None, None, :]
    block_top = lax.optimization_barrier(jnp.max(jnp.where(is_slot[..., None], row_top[:, :, None, :], -1e+30), axis=(0, 1)))
    ceiling = jnp.maximum(block_top, 0.0)
    spread = row_mass[:, :, None, :] * jnp.exp(row_top[:, :, None, :] - ceiling[None, None])
    block_mass = lax.optimization_barrier(jnp.sum(jnp.where(is_slot[..., None], spread, 0.0), axis=(0, 1)))
    row_norm = ceiling + jnp.log(jnp.exp(-ceiling) + block_mass)
    slot_norm = lax.optimization_barrier(jnp.sum(jnp.where(is_slot[..., None], row_norm[None, None], 0.0), axis=2))
    return (row_norm, slot_norm)

def reference(data_rows, centroids, block_mask, lower_bound):
    device_count = ROWS // ROW_DEV
    block_count = ROW_DEV // BLOCK
    shard_width = K // N_MP
    sharpness = 4.0 / math.sqrt(F)
    row_blocks = data_rows.reshape(device_count, block_count, BLOCK, F)
    dev_mask = block_mask.reshape(N_MP, device_count, block_count).transpose(1, 0, 2)
    slot_codes = jax.vmap(pack_codes)(dev_mask)
    cents = centroids.reshape(N_MP, shard_width, F)
    cent_norm = lax.optimization_barrier(jnp.sum(jnp.square(cents.astype(jnp.float32)), axis=2))

    def slot_rows_of(shard):
        code_s = lax.dynamic_index_in_dim(slot_codes, shard, 1, keepdims=False)
        taken = jax.vmap(lambda blk, cde: jnp.take(blk, jnp.maximum(cde - 1, 0), axis=0))(row_blocks, code_s)
        return (jnp.where((code_s > 0)[:, :, None, None], taken, jnp.zeros_like(taken)), code_s)

    def shard_scores(shard):
        slot_rows, code_s = slot_rows_of(shard)
        cent_s = lax.dynamic_index_in_dim(cents, shard, 0, keepdims=False)
        norm_s = lax.dynamic_index_in_dim(cent_norm, shard, 0, keepdims=False)
        products = jnp.dot(slot_rows.reshape(-1, F), cent_s.T, preferred_element_type=jnp.float32)
        scores = sharpness * (2.0 * products - norm_s[None, :])
        scores = scores.reshape(device_count, SLOTS, BLOCK, shard_width)
        is_valid = (code_s > 0)[:, :, None]
        best = lax.optimization_barrier(jnp.max(scores, axis=3))
        row_top = jnp.where(is_valid, best, -1e+30)
        row_mass = jnp.where(is_valid, lax.optimization_barrier(jnp.sum(jnp.exp(scores - best[..., None]), axis=3)), 0.0)
        return (scores, row_top, row_mass)
    all_scores, all_top, all_mass = lax.map(shard_scores, jnp.arange(N_MP, dtype=jnp.int32))
    row_norm, slot_norm = jax.vmap(combine_rows, in_axes=(0, 1, 1, None))(slot_codes, all_top, all_mass, block_count)

    def shard_sums(shard):
        slot_rows, code_s = slot_rows_of(shard)
        scores = lax.dynamic_index_in_dim(all_scores, shard, 0, keepdims=False)
        norm_s = lax.dynamic_index_in_dim(slot_norm, shard, 1, keepdims=False)
        is_valid = (code_s > 0)[:, :, None, None]
        weight = jnp.where(is_valid, jnp.exp(scores - norm_s[..., None]), 0.0)
        counts = lax.optimization_barrier(jnp.sum(weight, axis=(0, 1, 2)))
        weight_half = weight.astype(jnp.bfloat16).reshape(-1, shard_width)
        weighted = jnp.dot(weight_half.T, slot_rows.reshape(-1, F), preferred_element_type=jnp.float32)
        return (weighted, counts)
    weighted, counts = lax.map(shard_sums, jnp.arange(N_MP, dtype=jnp.int32))
    old_cents = cents.astype(jnp.float32)
    updated = (weighted + old_cents) / (counts[..., None] + 1.0)
    movement = jnp.sqrt(lax.optimization_barrier(jnp.sum(jnp.square(updated - old_cents), axis=2)) + 1.0)
    shard_peak = lax.optimization_barrier(jnp.max(movement, axis=1))
    new_lower = lower_bound - shard_peak[:, None]
    return (updated.reshape(K, F), movement.reshape(K), row_norm.reshape(ROWS), new_lower)
```

```python
import math

import jax
import jax.numpy as jnp
from jax import lax
from jax.sharding import PartitionSpec as P

BLOCK = 128


def swap(value, axis, size, offset):
    return lax.ppermute(value, axis, [(i, i ^ offset) for i in range(size)])


def on_device(data_rows, centroids, block_mask, lower_bound):
    feat = data_rows.shape[1]
    width = centroids.shape[0]
    block_count = data_rows.shape[0] // BLOCK
    n_mp = lax.axis_size("mp")
    n_dp = lax.axis_size("dp")
    own_width = width // n_dp
    my_mp = lax.axis_index("mp")
    my_dp = lax.axis_index("dp")
    sharpness = 4.0 / math.sqrt(feat)

    labels = jnp.arange(1, block_count + 1, dtype=jnp.int32)
    codes = jnp.sum(block_mask * labels[None, :], axis=1)

    def outgoing(k):
        code = lax.dynamic_index_in_dim(codes, my_mp ^ k, 0, keepdims=False)
        start = jnp.maximum(code - 1, 0) * BLOCK
        return lax.dynamic_slice(data_rows, (start, 0), (BLOCK, feat))

    order = list(range(2, n_mp)) + [1]
    got = {0: outgoing(0)}
    for k in order:
        got[k] = swap(outgoing(k), "mp", n_mp, k)

    cent_norm = jnp.sum(jnp.square(centroids.astype(jnp.float32)), axis=1)

    scores, lses = {}, {}
    groups = [(k, k + 1) for k in range(0, n_mp, 2)]
    for group in groups:
        rows = jnp.concatenate([got[k] for k in group], axis=0)
        product = lax.dot_general(
            centroids, rows, (((1,), (1,)), ((), ())), preferred_element_type=jnp.float32
        )
        score = sharpness * (2.0 * product - cent_norm[:, None])
        top = jnp.max(score, axis=0)
        lse = top + jnp.log(jnp.sum(jnp.exp(score - top[None, :]), axis=0))
        scores[group] = score
        for i, k in enumerate(group):
            lses[k] = lse[i * BLOCK : (i + 1) * BLOCK]

    note = jnp.concatenate(
        [
            jnp.stack([lses[k] for k in range(n_mp)]),
            jnp.pad(codes.astype(jnp.float32), (0, BLOCK - n_mp))[None, :],
        ]
    )
    notes = lax.all_to_all(
        jnp.broadcast_to(note[None], (n_mp,) + note.shape), "mp", split_axis=0, concat_axis=0, tiled=True
    )
    shard_ids = jnp.arange(n_mp, dtype=jnp.int32)
    lse_of = notes[:, :n_mp, :]
    all_code = notes[:, n_mp, :n_mp].astype(jnp.int32)
    all_lse = lse_of[shard_ids[None, :], shard_ids[None, :] ^ shard_ids[:, None]]
    tops = jnp.where((all_code > 0)[:, :, None], all_lse, -1e30)

    def normalizer(same, lse):
        kept = jnp.where(same[:, :, None], lse, -1e30)
        peak = jnp.maximum(jnp.max(kept, axis=1), 0.0)
        mass = jnp.sum(jnp.exp(kept - peak[:, None, :]), axis=1)
        return peak + jnp.log(jnp.exp(-peak) + mass)

    my_lse = lax.dynamic_index_in_dim(tops, my_mp, 0, keepdims=False)
    row_norm = normalizer(codes[None, :] == labels[:, None], jnp.broadcast_to(my_lse[None], (block_count,) + my_lse.shape))
    log_norm = row_norm.reshape(-1)

    slot_code = lax.dynamic_index_in_dim(all_code, my_mp, 1, keepdims=False)
    slot_norm = normalizer((all_code == slot_code[:, None]) & (all_code > 0), tops)

    weights, counts = [], 0.0
    for group in groups:
        src = [my_mp ^ k for k in group]
        norm = jnp.concatenate([slot_norm[m] for m in src])
        valid = jnp.concatenate([jnp.broadcast_to(slot_code[m] > 0, (BLOCK,)) for m in src])
        weight = jnp.where(valid[None, :], jnp.exp(scores[group] - norm[None, :]), 0.0)
        counts = counts + jnp.sum(weight, axis=1)
        weights.append(weight.astype(jnp.bfloat16))
    weight_half = jnp.concatenate(weights, axis=1)
    rows = jnp.concatenate([got[k] for k in range(n_mp)], axis=0)

    def quarter(j):
        return (my_dp ^ j) * own_width

    def partial(j, half):
        w = lax.dynamic_slice(weight_half, (quarter(j), 0), (own_width, weight_half.shape[1]))
        x = lax.slice_in_dim(rows, half * (feat // 2), (half + 1) * (feat // 2), axis=1)
        return lax.dot_general(w, x, (((1,), (0,)), ((), ())), preferred_element_type=jnp.float32)

    count_of = {0: counts}
    for j in range(1, n_dp):
        count_of[j] = swap(counts, "dp", n_dp, j)

    def sub(vec, j):
        return lax.dynamic_slice(vec, (quarter(j),), (own_width,))

    def scale(members, j):
        total = sum(sub(count_of[i], j) for i in members)
        return jnp.maximum(total, 2.0**-20)[:, None] * 2.0**-10

    bits = [1 << b for b in range(n_dp.bit_length() - 1)]
    halves = []
    plan = [bits, bits[::-1]]
    current = [{}, {}]
    for j in reversed(range(n_dp)):
        for half in range(2):
            jj = j if half == 0 or n_dp != 4 else {3: 3, 1: 2, 2: 1, 0: 0}[j]
            current[half][jj] = None
    todo = [[j for j in reversed(range(n_dp))] for _ in range(2)]
    for half in range(2):
        for j in todo[half]:
            current[half][j] = partial(j, half)
    members = [{0}, {0}]
    for step in range(len(bits)):
        for half in range(2):
            bit = plan[half][step]
            cur = current[half]
            mine = members[half]
            theirs = {i ^ bit for i in mine}
            kept = {}
            for j in sorted(cur, reverse=True):
                if not j & bit:
                    continue
                sent = (cur[j] / scale(mine, j)).astype(jnp.float16)
                back = swap(sent, "dp", n_dp, bit)
                kept[j ^ bit] = cur[j ^ bit] + back.astype(jnp.float32) * scale(theirs, j ^ bit)
            current[half] = kept
            members[half] = mine | theirs
    part_sums = jnp.concatenate([current[0][0], current[1][0]], axis=1)
    part_counts = sum(sub(count_of[j], 0) for j in range(n_dp))

    old_cents = lax.dynamic_slice_in_dim(centroids, my_dp * own_width, own_width, 0).astype(jnp.float32)
    updated = (part_sums + old_cents) / (part_counts[:, None] + 1.0)
    movement = jnp.sqrt(jnp.sum(jnp.square(updated - old_cents), axis=1) + 1.0)
    peak = jnp.broadcast_to(jnp.max(movement), (n_dp * n_mp, 1))
    shard_peaks = lax.all_to_all(peak, ("dp", "mp"), split_axis=0, concat_axis=0, tiled=True)
    shard_peak = jnp.max(shard_peaks.reshape(n_dp, n_mp), axis=0)
    new_lower = lower_bound - shard_peak[:, None]
    return (updated, movement, log_norm, new_lower)


def solution(mesh):
    placed = (P(("dp", "mp"), None), P("mp", None), P(None, ("dp", "mp")), P(None, ("dp", "mp")))
    return jax.shard_map(
        on_device,
        mesh=mesh,
        in_specs=placed,
        out_specs=(P(("mp", "dp"), None), P(("mp", "dp")), P(("dp", "mp")), P(None, ("dp", "mp"))),
        check_vma=False,
    )
```

```python
import math

import jax
import jax.numpy as jnp
from jax import lax
from jax.experimental import pallas as pl
from jax.experimental.pallas import tpu as pltpu
from jax.sharding import PartitionSpec as P


BLOCK = 128
LANES = 128
F32 = jnp.float32
BF16 = jnp.bfloat16
NEVER = 1e30
ANY = pl.BlockSpec(memory_space=pl.ANY)
SMEM = pl.BlockSpec(memory_space=pltpu.SMEM)
VMEM = pl.BlockSpec(memory_space=pltpu.VMEM)


def hbm(*arrays):
    return [pltpu.with_memory_space_constraint(v, pltpu.HBM) for v in arrays]


def vmem(*arrays):
    return [pltpu.with_memory_space_constraint(v, pltpu.VMEM) for v in arrays]


def swap(value, axis, size, offset):
    return lax.ppermute(value, axis, [(i, i ^ offset) for i in range(size)])


def call(body, out_shape, in_specs, out_specs, scratch=(), vmem=4):
    return pl.pallas_call(
        body,
        out_shape=out_shape,
        in_specs=in_specs,
        out_specs=out_specs,
        scratch_shapes=list(scratch),
        compiler_params=pltpu.CompilerParams(vmem_limit_bytes=vmem << 20),
    )


def take_slots(ids, mask_t, data_rows, pieces, with_codes):
    block_count, n_mp = mask_t.shape

    def body(ids_ref, mask_ref, rows_ref, *refs):
        outs, sems = refs[:-1], refs[-1]

        def code_of(k):
            shard = ids_ref[0] ^ k
            code = mask_ref[0, shard]
            for b in range(1, block_count):
                code = code + (b + 1) * mask_ref[b, shard]
            return code

        copies = []
        for i, (k, first, count) in enumerate(pieces):
            start = jnp.maximum(code_of(k) - 1, 0) * BLOCK
            src = rows_ref.at[pl.ds(pl.multiple_of(start, BLOCK), BLOCK), pl.ds(first, count)]
            copies.append(pltpu.make_async_copy(src, outs[i], sems.at[i]))
            copies[-1].start()
        if with_codes:
            for k in range(n_mp):
                outs[-1][k : k + 1, :] = jnp.full((1, LANES), code_of(k), jnp.int32).astype(F32)
        for copy in copies:
            copy.wait()

    shapes = [pltpu.VMEM((BLOCK, count), data_rows.dtype) for _, _, count in pieces]
    if with_codes:
        shapes.append(jax.ShapeDtypeStruct((n_mp, LANES), F32))
    return call(
        body, shapes, [SMEM, SMEM, ANY], [VMEM] * len(shapes), [pltpu.SemaphoreType.DMA((len(pieces),))], 8
    )(ids, mask_t, *hbm(data_rows))


def load_centroids(centroids, n_parts):
    width, feat = centroids.shape
    part = width // n_parts

    def body(in_ref, out_ref, norm_ref):
        values = in_ref[...]
        out_ref[...] = values
        norm_ref[...] = jnp.sum(jnp.square(values.astype(F32)), axis=1, keepdims=True)

    return pl.pallas_call(
        body,
        out_shape=[pltpu.VMEM((width, feat), centroids.dtype), jax.ShapeDtypeStruct((width, 1), F32)],
        grid=(n_parts,),
        in_specs=[pl.BlockSpec((part, feat), lambda i: (i, 0))],
        out_specs=[pl.BlockSpec((part, feat), lambda i: (i, 0)), pl.BlockSpec((part, 1), lambda i: (i, 0))],
        name="load_centroids",
        compiler_params=pltpu.CompilerParams(vmem_limit_bytes=10 << 20),
    )(*hbm(centroids))


def product(cents_ref, rows_ref):
    return lax.dot_general(
        cents_ref[...], rows_ref[...], (((1,), (1,)), ((), ())), preferred_element_type=F32
    )


def keep(row_refs, pieces, out_ref):
    for ref, (place, first, count) in zip(row_refs, pieces):
        out_ref[place * BLOCK : (place + 1) * BLOCK, first : first + count] = ref[...]


def own_scores(ids, centroids, cent_norm, rows, pieces, state, at, n_slots, n_parts, sharpness):
    width, feat = centroids.shape
    part = width // n_parts
    n_rows = n_slots * BLOCK
    fresh = isinstance(state[0], jax.ShapeDtypeStruct)
    n_in = len(rows)

    def body(ids_ref, cents_ref, norm_ref, *refs):
        row_refs = refs[:n_in]
        rows_out, score_out, lse_out, top_ref, mass_ref = refs[len(refs) - 5 :]
        step = pl.program_id(0)

        @pl.when(step == 0)
        def _():
            keep(row_refs, pieces, rows_out)
            top_ref[...] = jnp.full(top_ref.shape, -NEVER, F32)
            mass_ref[...] = jnp.zeros(mass_ref.shape, F32)

        score = sharpness * (2.0 * product(cents_ref, rows_out) - norm_ref[...])

        @pl.when(step == ids_ref[1])
        def _():
            score_out[...] = score

        old_top = top_ref[...]
        top = jnp.maximum(old_top, jnp.max(score, axis=0, keepdims=True))
        mass = mass_ref[...] * jnp.exp(old_top - top) + jnp.sum(jnp.exp(score - top), axis=0, keepdims=True)
        top_ref[...] = top
        mass_ref[...] = mass
        lse = top + jnp.log(mass)
        for i in range(n_slots):
            lse_out[i] = lse[:, i * BLOCK : (i + 1) * BLOCK]

    grid_spec = pltpu.PrefetchScalarGridSpec(
        num_scalar_prefetch=1,
        grid=(n_parts,),
        in_specs=[
            pl.BlockSpec((part, feat), lambda i, ids: (i, 0)),
            pl.BlockSpec((part, 1), lambda i, ids: (i, 0)),
        ]
        + [pl.BlockSpec(r.shape, lambda i, ids: (0, 0)) for r in rows]
        + ([] if fresh else [ANY] * 3),
        out_specs=[
            pl.BlockSpec((n_rows, feat), lambda i, ids: (at, 0)),
            pl.BlockSpec((part, n_rows), lambda i, ids: (0, at)),
            pl.BlockSpec((n_slots, 1, BLOCK), lambda i, ids: (at, 0, 0)),
        ],
        scratch_shapes=[pltpu.VMEM((1, n_rows), F32)] * 2,
    )
    return pl.pallas_call(
        body,
        out_shape=[pltpu.VMEM(v.shape, v.dtype) for v in state],
        grid_spec=grid_spec,
        input_output_aliases={} if fresh else {3 + n_in + i: i for i in range(3)},
        name="own_scores",
        compiler_params=pltpu.CompilerParams(vmem_limit_bytes=10 << 20),
    )(ids, *vmem(centroids), cent_norm, *rows, *([] if fresh else state))


def side_scores(ids, centroids, cent_norm, sides, pieces, state, at, n_slots, half, sharpness):
    feat = centroids.shape[1]
    n_rows = n_slots * BLOCK
    fresh = isinstance(state[0], jax.ShapeDtypeStruct)
    n_in = len(sides[0])

    def body(ids_ref, cents_ref, norm_ref, *refs):
        x_refs, y_refs = refs[:n_in], refs[n_in : 2 * n_in]
        x_rows, y_rows, x_out, y_out = refs[len(refs) - 4 :]
        step = pl.program_id(0)

        def score(rows_ref):
            return sharpness * (2.0 * product(cents_ref, rows_ref) - norm_ref[...])

        @pl.when(step == 0)
        def _():
            keep(x_refs, pieces, x_rows)
            keep(y_refs, pieces, y_rows)

        @pl.when(step != 3)
        def _():
            x_out[...] = score(x_rows)

        @pl.when(step != 2)
        def _():
            y_out[...] = score(y_rows)

    def block(i, ids):
        mine = ids[1]
        other = jnp.where(i == 2, 2 * (mine ^ 2) + 1, 2 * (mine ^ 1))
        return (jnp.where(i < 2, 2 * mine + i, other), 0)

    grid_spec = pltpu.PrefetchScalarGridSpec(
        num_scalar_prefetch=1,
        grid=(4,),
        in_specs=[pl.BlockSpec((half, feat), block), pl.BlockSpec((half, 1), block)]
        + [pl.BlockSpec(r.shape, lambda i, ids: (0, 0)) for r in sides[0] + sides[1]]
        + ([] if fresh else [ANY] * 4),
        out_specs=[
            pl.BlockSpec((n_rows, feat), lambda i, ids: (at, 0)),
            pl.BlockSpec((n_rows, feat), lambda i, ids: (at, 0)),
            pl.BlockSpec((half, n_rows), lambda i, ids: (jnp.minimum(i, 2), at)),
            pl.BlockSpec((half, n_rows), lambda i, ids: (jnp.where(i == 3, 2, jnp.minimum(i, 1)), at)),
        ],
    )
    return pl.pallas_call(
        body,
        out_shape=[pltpu.VMEM(v.shape, v.dtype) for v in state],
        grid_spec=grid_spec,
        input_output_aliases={} if fresh else {3 + 2 * n_in + i: i for i in range(4)},
        name="side_scores",
        compiler_params=pltpu.CompilerParams(vmem_limit_bytes=12 << 20),
    )(ids, *vmem(centroids), cent_norm, *sides[0], *sides[1], *([] if fresh else state))


def log_total(kept):
    peak = jnp.maximum(jnp.max(kept, axis=0, keepdims=True), 0.0)
    mass = jnp.sum(jnp.exp(kept - peak), axis=0, keepdims=True)
    return peak + jnp.log(jnp.exp(-peak) + mass)


def combine(notes, block_count):
    n_mp = len(notes)

    def body(*refs):
        note_refs, (slot_ref, row_ref) = refs[:n_mp], refs[n_mp:]
        for k in range(n_mp):
            lse = jnp.concatenate([note_refs[k ^ j][j : j + 1, :] for j in range(n_mp)], axis=0)
            code = note_refs[k][n_mp : 2 * n_mp, :]
            mine = code[k : k + 1, :]
            total = log_total(jnp.where((code == mine) & (code > 0.0), lse, -NEVER))
            slot_ref[k : k + 1, :] = jnp.where(mine > 0.0, total, NEVER)
            if k == 0:
                for b in range(block_count):
                    row_ref[b : b + 1, :] = log_total(jnp.where(code == float(b + 1), lse, -NEVER))

    return call(
        body,
        [jax.ShapeDtypeStruct((n_mp, LANES), F32), jax.ShapeDtypeStruct((block_count, LANES), F32)],
        [VMEM] * n_mp,
        [VMEM, VMEM],
    )(*notes)


def weights_of(score_ref, norm_ref, into, column, total):
    for k in range(norm_ref.shape[0]):
        tile = jnp.exp(score_ref[:, k * BLOCK : (k + 1) * BLOCK] - norm_ref[k : k + 1, :])
        total = tile if total is None else total + tile
        into[:, column + k * BLOCK : column + (k + 1) * BLOCK] = tile.astype(BF16)
    return total


def sent_sums(side_rows, side_score, norms, half, first, columns, tile):
    n_rows = side_rows[0].shape[0]
    steps = columns // tile

    def body(x_ref, y_ref, xs_ref, ys_ref, xn_ref, yn_ref, x_out, y_out, w_buf, c_buf):
        step = pl.program_id(0)

        @pl.when(step == 0)
        def _():
            for i, (s_ref, n_ref) in enumerate(((xs_ref, xn_ref), (ys_ref, yn_ref))):
                total = weights_of(s_ref, n_ref, w_buf.at[i], 0, None)
                c_buf[i] = jnp.broadcast_to(jnp.sum(total, axis=1, keepdims=True), c_buf.shape[1:])

        for i, (r_ref, out) in enumerate(((x_ref, x_out), (y_ref, y_out))):
            counts = c_buf[i]

            @pl.when(step < steps)
            def _():
                part = jnp.dot(w_buf[i], r_ref[...], preferred_element_type=F32)
                out[...] = part * (2.0**10 / jnp.maximum(counts[:, 0:1], 2.0**-20))

            @pl.when(step == steps)
            def _():
                hi = counts.astype(BF16).astype(F32)
                mid = (counts - hi).astype(BF16).astype(F32)
                low = (counts - hi - mid).astype(BF16).astype(F32)
                lane = lax.broadcasted_iota(jnp.int32, counts.shape, 1)
                terms = jnp.where(lane == 0, hi, jnp.where(lane == 1, mid, jnp.where(lane == 2, low, 0.0)))
                out[:, :LANES] = terms

    base = first // tile
    rows_spec = pl.BlockSpec((n_rows, tile), lambda i: (0, base + jnp.minimum(i, steps - 1)))
    score_spec = pl.BlockSpec((half, n_rows), lambda i: (2, 0))
    norm_spec = pl.BlockSpec(norms[0].shape, lambda i: (0, 0))
    out_spec = pl.BlockSpec((half, tile), lambda i: (0, i))
    with_counts = first == 0
    width = columns + LANES if with_counts else columns
    return pl.pallas_call(
        body,
        out_shape=[jax.ShapeDtypeStruct((half, width), F32)] * 2,
        grid=(steps + 1 if with_counts else steps,),
        in_specs=[rows_spec] * 2 + [score_spec] * 2 + [norm_spec] * 2,
        out_specs=[out_spec] * 2,
        scratch_shapes=[pltpu.VMEM((2, half, n_rows), BF16), pltpu.VMEM((2, half, LANES), F32)],
        name="sent_sums",
        compiler_params=pltpu.CompilerParams(vmem_limit_bytes=16 << 20),
    )(*vmem(*side_rows, *side_score), *norms)


def own_sums(rows, scores, norms, width, tile):
    n_rows, feat = rows[0].shape

    def body(a_ref, b_ref, c_ref, as_ref, bs_ref, cs_ref, an_ref, bn_ref, cn_ref, out_ref, count_ref, w_buf):
        @pl.when(pl.program_id(0) == 0)
        def _():
            total = None
            for i, (s_ref, n_ref) in enumerate(((as_ref, an_ref), (bs_ref, bn_ref), (cs_ref, cn_ref))):
                total = weights_of(s_ref, n_ref, w_buf, i * n_rows, total)
            count_ref[...] = jnp.sum(total, axis=1, keepdims=True)

        acc = jnp.dot(w_buf[:, :n_rows], a_ref[...], preferred_element_type=F32)
        acc += jnp.dot(w_buf[:, n_rows : 2 * n_rows], b_ref[...], preferred_element_type=F32)
        acc += jnp.dot(w_buf[:, 2 * n_rows :], c_ref[...], preferred_element_type=F32)
        out_ref[...] = acc

    return pl.pallas_call(
        body,
        out_shape=[pltpu.VMEM((width, feat), F32), jax.ShapeDtypeStruct((width, 1), F32)],
        grid=(feat // tile,),
        in_specs=[pl.BlockSpec((n_rows, tile), lambda i: (0, i))] * 3
        + [pl.BlockSpec((width, n_rows), lambda i: (0, 0))] * 3
        + [pl.BlockSpec(norms[0].shape, lambda i: (0, 0))] * 3,
        out_specs=[
            pl.BlockSpec((width, tile), lambda i: (0, i)),
            pl.BlockSpec((width, 1), lambda i: (0, 0)),
        ],
        scratch_shapes=[pltpu.VMEM((width, 3 * n_rows), BF16)],
        name="own_sums",
        compiler_params=pltpu.CompilerParams(vmem_limit_bytes=24 << 20),
    )(*vmem(*rows, *scores), *norms)


def update(ids, own, counts, parts, centroids, first, state, n_devices):
    width, feat = own.shape
    half = width // 2
    columns = feat // 2
    lead = first == 0
    rows = half // 2
    steps = half // rows

    def body(ids_ref, own_ref, count_ref, a_ref, b_ref, old_ref, *refs):
        step = pl.program_id(0)

        def finish(part_ref):
            if lead:
                new_ref, sent_ref, square_ref = refs
                tail = part_ref[:, columns:]
                lane = lax.broadcasted_iota(jnp.int32, tail.shape, 1)
                sent = jnp.sum(jnp.where(lane < 3, tail, 0.0), axis=1, keepdims=True)
                sent_ref[...] = sent
            else:
                sent_in, square_in, _, new_ref, move_ref, peak_ref = refs
                sent = sent_in[...]
            back = part_ref[:, :columns] * (jnp.maximum(sent, 2.0**-20) * 2.0**-10)
            before = old_ref[...].astype(F32)
            after = (own_ref[...] + back + before) / (count_ref[...] + sent + 1.0)
            new_ref[...] = after
            square = jnp.sum(jnp.square(after - before), axis=1, keepdims=True)
            if lead:
                square_ref[...] = square
            else:
                move = jnp.sqrt(square + square_in[...] + 1.0)
                move_ref[...] = move
                top = jnp.broadcast_to(jnp.max(move, axis=0, keepdims=True), peak_ref.shape)
                peak_ref[...] = jnp.where(step == 0, top, jnp.maximum(top, peak_ref[...]))

        @pl.when(step < steps)
        def _():
            finish(a_ref)

        @pl.when(step >= steps)
        def _():
            finish(b_ref)

    at = 0 if lead else 1
    column = pl.BlockSpec((rows, 1), lambda i, ids: (i, 0))
    part_width = parts[0].shape[1]
    in_specs = [
        pl.BlockSpec((rows, columns), lambda i, ids: (i, at)),
        column,
        pl.BlockSpec((rows, part_width), lambda i, ids: (jnp.minimum(i, steps - 1), 0)),
        pl.BlockSpec((rows, part_width), lambda i, ids: (jnp.maximum(i - steps, 0), 0)),
        pl.BlockSpec((rows, columns), lambda i, ids: (ids[1] * (2 * steps) + i, at)),
    ]
    new_spec = pl.BlockSpec((rows, columns), lambda i, ids: (i, at))
    new_shape = jax.ShapeDtypeStruct((width, feat), F32)
    thin = jax.ShapeDtypeStruct((width, 1), F32)
    if lead:
        out_shape, out_specs, extra, aliases = [new_shape, thin, thin], [new_spec, column, column], [], {}
    else:
        new, sent, square = state
        extra = [sent, square, new]
        in_specs += [column, column, ANY]
        out_shape = [new_shape, thin, jax.ShapeDtypeStruct((n_devices, LANES), F32)]
        out_specs = [new_spec, column, pl.BlockSpec((n_devices, LANES), lambda i, ids: (0, 0))]
        aliases = {8: 0}
    return pl.pallas_call(
        body,
        out_shape=out_shape,
        grid_spec=pltpu.PrefetchScalarGridSpec(
            num_scalar_prefetch=1, grid=(2 * steps,), in_specs=in_specs, out_specs=out_specs
        ),
        input_output_aliases=aliases,
        name="update",
        compiler_params=pltpu.CompilerParams(vmem_limit_bytes=8 << 20),
    )(ids, *vmem(own), counts, *parts, *vmem(centroids), *extra)


def z_order(n_mp):
    half = n_mp // 2
    return [half] + [k for k in range(2, n_mp) if k != half]


def own_groups(n_mp):
    return [(k, k + 1) for k in range(0, n_mp, 2)]


def on_square(data_rows, centroids, block_mask, lower_bound):
    feat = data_rows.shape[1]
    width = centroids.shape[0]
    block_count = data_rows.shape[0] // BLOCK
    n_mp = lax.axis_size("mp")
    n_dp = lax.axis_size("dp")
    own_width = width // n_dp
    half = own_width // 2
    my_mp = lax.axis_index("mp").astype(jnp.int32)
    my_dp = lax.axis_index("dp").astype(jnp.int32)
    sharpness = 4.0 / math.sqrt(feat)
    ids = jnp.stack([my_mp, my_dp])
    mask_t = block_mask.T

    last = n_mp - 1
    cuts = {k: [(k, 0, feat)] for k in range(n_mp)}
    cuts[last] = [(last, 0, feat // 2), (last, feat // 2, feat // 2)]
    early = [p for k in z_order(n_mp)[:3] for p in cuts[k]]
    late = cuts[0] + [p for k in z_order(n_mp)[3:] for p in cuts[k]] + cuts[1]
    got = dict(zip(early, take_slots(ids, mask_t, data_rows, early, False)))
    *rest, codes = take_slots(ids, mask_t, data_rows, late, True)
    got.update(zip(late, rest))
    for piece in early + late[1:]:
        got[piece] = swap(got[piece], "mp", n_mp, piece[0])

    side = {}
    for k in range(n_mp):
        for piece in cuts[k]:
            for bit in (1, 2):
                side[bit, piece] = swap(got[piece], "dp", n_dp, bit)

    cents, cent_norm = load_centroids(centroids, 2 * n_dp)

    n_rows = n_mp * BLOCK
    own = [
        jax.ShapeDtypeStruct((n_rows, feat), BF16),
        jax.ShapeDtypeStruct((own_width, n_rows), F32),
        jax.ShapeDtypeStruct((n_mp, 1, BLOCK), F32),
    ]
    sides = [jax.ShapeDtypeStruct((n_rows, feat), BF16)] * 2
    sides += [jax.ShapeDtypeStruct((3 * half, n_rows), F32)] * 2
    for group in own_groups(n_mp):
        held = [p for k in group for p in cuts[k]]
        placed = [(p[0] - group[0], p[1], p[2]) for p in held]
        own = own_scores(
            ids, cents, cent_norm, [got[p] for p in held], placed, own, group[0] // len(group), len(group),
            n_dp, sharpness,
        )
    for i in range(n_mp // 2):
        held = cuts[2 * i] + cuts[2 * i + 1]
        placed = [(p[0] - 2 * i, p[1], p[2]) for p in held]
        pair = [[side[bit, p] for p in held] for bit in (1, 2)]
        sides = side_scores(ids, cents, cent_norm, pair, placed, sides, i, 2, half, sharpness)

    note = jnp.concatenate([own[2][:, 0, :], codes])
    notes = [note]
    for k in range(1, n_mp):
        notes.append(swap(note, "mp", n_mp, k))
    slot_norm, row_norm = combine(notes, block_count)
    log_norm = row_norm.reshape(-1)
    side_norm = []
    for bit in (1, 2):
        side_norm.append(swap(slot_norm, "dp", n_dp, bit))

    received = []
    for part in range(2):
        first = part * (feat // 2)
        sent = sent_sums(sides[:2], sides[2:], side_norm, half, first, feat // 2, feat // 4)
        for_y, for_x = [v.astype(jnp.float16) for v in sent]
        received.append([swap(for_x, "dp", n_dp, 1), swap(for_y, "dp", n_dp, 2)])
    total, counts = own_sums(
        [own[0], sides[0], sides[1]],
        [own[1], sides[2], sides[3]],
        [slot_norm] + side_norm,
        own_width,
        feat // 4,
    )
    state = None
    for part in range(2):
        parts = [v.astype(F32) for v in received[part]]
        state = update(ids, total, counts, parts, cents, part * (feat // 2), state, n_dp * n_mp)
    updated, movement, peak = state
    shard_peaks = lax.all_to_all(peak, ("dp", "mp"), split_axis=0, concat_axis=0, tiled=True)
    shard_peak = jnp.max(shard_peaks.reshape(n_dp, n_mp, LANES), axis=(0, 2))
    new_lower = lower_bound - shard_peak[:, None]
    return (updated, movement[:, 0], log_norm, new_lower)


def on_device(data_rows, centroids, block_mask, lower_bound):
    feat = data_rows.shape[1]
    width = centroids.shape[0]
    block_count = data_rows.shape[0] // BLOCK
    n_mp = lax.axis_size("mp")
    n_dp = lax.axis_size("dp")
    own_width = width // n_dp
    my_mp = lax.axis_index("mp")
    my_dp = lax.axis_index("dp")
    sharpness = 4.0 / math.sqrt(feat)

    labels = jnp.arange(1, block_count + 1, dtype=jnp.int32)
    codes = jnp.sum(block_mask * labels[None, :], axis=1)

    def outgoing(k):
        code = lax.dynamic_index_in_dim(codes, my_mp ^ k, 0, keepdims=False)
        start = jnp.maximum(code - 1, 0) * BLOCK
        return lax.dynamic_slice(data_rows, (start, 0), (BLOCK, feat))

    order = list(range(2, n_mp)) + [1]
    got = {0: outgoing(0)}
    for k in order:
        got[k] = swap(outgoing(k), "mp", n_mp, k)

    cent_norm = jnp.sum(jnp.square(centroids.astype(jnp.float32)), axis=1)

    scores, lses = {}, {}
    groups = [(k, k + 1) for k in range(0, n_mp, 2)]
    for group in groups:
        rows = jnp.concatenate([got[k] for k in group], axis=0)
        product = lax.dot_general(
            centroids, rows, (((1,), (1,)), ((), ())), preferred_element_type=jnp.float32
        )
        score = sharpness * (2.0 * product - cent_norm[:, None])
        top = jnp.max(score, axis=0)
        lse = top + jnp.log(jnp.sum(jnp.exp(score - top[None, :]), axis=0))
        scores[group] = score
        for i, k in enumerate(group):
            lses[k] = lse[i * BLOCK : (i + 1) * BLOCK]

    note = jnp.concatenate(
        [
            jnp.stack([lses[k] for k in range(n_mp)]),
            jnp.pad(codes.astype(jnp.float32), (0, BLOCK - n_mp))[None, :],
        ]
    )
    notes = lax.all_to_all(
        jnp.broadcast_to(note[None], (n_mp,) + note.shape), "mp", split_axis=0, concat_axis=0, tiled=True
    )
    shard_ids = jnp.arange(n_mp, dtype=jnp.int32)
    lse_of = notes[:, :n_mp, :]
    all_code = notes[:, n_mp, :n_mp].astype(jnp.int32)
    all_lse = lse_of[shard_ids[None, :], shard_ids[None, :] ^ shard_ids[:, None]]
    tops = jnp.where((all_code > 0)[:, :, None], all_lse, -1e30)

    def normalizer(same, lse):
        kept = jnp.where(same[:, :, None], lse, -1e30)
        peak = jnp.maximum(jnp.max(kept, axis=1), 0.0)
        mass = jnp.sum(jnp.exp(kept - peak[:, None, :]), axis=1)
        return peak + jnp.log(jnp.exp(-peak) + mass)

    my_lse = lax.dynamic_index_in_dim(tops, my_mp, 0, keepdims=False)
    row_norm = normalizer(codes[None, :] == labels[:, None], jnp.broadcast_to(my_lse[None], (block_count,) + my_lse.shape))
    log_norm = row_norm.reshape(-1)

    slot_code = lax.dynamic_index_in_dim(all_code, my_mp, 1, keepdims=False)
    slot_norm = normalizer((all_code == slot_code[:, None]) & (all_code > 0), tops)

    weights, counts = [], 0.0
    for group in groups:
        src = [my_mp ^ k for k in group]
        norm = jnp.concatenate([slot_norm[m] for m in src])
        valid = jnp.concatenate([jnp.broadcast_to(slot_code[m] > 0, (BLOCK,)) for m in src])
        weight = jnp.where(valid[None, :], jnp.exp(scores[group] - norm[None, :]), 0.0)
        counts = counts + jnp.sum(weight, axis=1)
        weights.append(weight.astype(jnp.bfloat16))
    weight_half = jnp.concatenate(weights, axis=1)
    rows = jnp.concatenate([got[k] for k in range(n_mp)], axis=0)

    def quarter(j):
        return (my_dp ^ j) * own_width

    def partial(j, half):
        w = lax.dynamic_slice(weight_half, (quarter(j), 0), (own_width, weight_half.shape[1]))
        x = lax.slice_in_dim(rows, half * (feat // 2), (half + 1) * (feat // 2), axis=1)
        return lax.dot_general(w, x, (((1,), (0,)), ((), ())), preferred_element_type=jnp.float32)

    count_of = {0: counts}
    for j in range(1, n_dp):
        count_of[j] = swap(counts, "dp", n_dp, j)

    def sub(vec, j):
        return lax.dynamic_slice(vec, (quarter(j),), (own_width,))

    def scale(members, j):
        total = sum(sub(count_of[i], j) for i in members)
        return jnp.maximum(total, 2.0**-20)[:, None] * 2.0**-10

    bits = [1 << b for b in range(n_dp.bit_length() - 1)]
    plan = [bits, bits[::-1]]
    current = [{}, {}]
    for j in reversed(range(n_dp)):
        for half in range(2):
            jj = j if half == 0 or n_dp != 4 else {3: 3, 1: 2, 2: 1, 0: 0}[j]
            current[half][jj] = None
    todo = [[j for j in reversed(range(n_dp))] for _ in range(2)]
    for half in range(2):
        for j in todo[half]:
            current[half][j] = partial(j, half)
    members = [{0}, {0}]
    for step in range(len(bits)):
        for half in range(2):
            bit = plan[half][step]
            cur = current[half]
            mine = members[half]
            theirs = {i ^ bit for i in mine}
            kept = {}
            for j in sorted(cur, reverse=True):
                if not j & bit:
                    continue
                sent = (cur[j] / scale(mine, j)).astype(jnp.float16)
                back = swap(sent, "dp", n_dp, bit)
                kept[j ^ bit] = cur[j ^ bit] + back.astype(jnp.float32) * scale(theirs, j ^ bit)
            current[half] = kept
            members[half] = mine | theirs
    part_sums = jnp.concatenate([current[0][0], current[1][0]], axis=1)
    part_counts = sum(sub(count_of[j], 0) for j in range(n_dp))

    old_cents = lax.dynamic_slice_in_dim(centroids, my_dp * own_width, own_width, 0).astype(jnp.float32)
    updated = (part_sums + old_cents) / (part_counts[:, None] + 1.0)
    movement = jnp.sqrt(jnp.sum(jnp.square(updated - old_cents), axis=1) + 1.0)
    peak = jnp.broadcast_to(jnp.max(movement), (n_dp * n_mp, 1))
    shard_peaks = lax.all_to_all(peak, ("dp", "mp"), split_axis=0, concat_axis=0, tiled=True)
    shard_peak = jnp.max(shard_peaks.reshape(n_dp, n_mp), axis=0)
    new_lower = lower_bound - shard_peak[:, None]
    return (updated, movement, log_norm, new_lower)


def solution(mesh):
    placed = (P(("dp", "mp"), None), P("mp", None), P(None, ("dp", "mp")), P(None, ("dp", "mp")))
    square = mesh.shape["dp"] == 4

    def body(*args):
        return on_square(*args) if square else on_device(*args)

    return jax.shard_map(
        body,
        mesh=mesh,
        in_specs=placed,
        out_specs=(P(("mp", "dp"), None), P(("mp", "dp")), P(("dp", "mp")), P(None, ("dp", "mp"))),
        check_vma=False,
    )
```

```python
import math

import jax
import jax.numpy as jnp
from jax import lax
from jax.experimental import pallas as pl
from jax.experimental.pallas import tpu as pltpu
from jax.sharding import PartitionSpec as P


BLOCK = 128
LANES = 128
F32 = jnp.float32
BF16 = jnp.bfloat16
NEVER = 1e30
ANY = pl.BlockSpec(memory_space=pl.ANY)
SMEM = pl.BlockSpec(memory_space=pltpu.SMEM)
VMEM = pl.BlockSpec(memory_space=pltpu.VMEM)


def hbm(*arrays):
    return [pltpu.with_memory_space_constraint(v, pltpu.HBM) for v in arrays]


def vmem(*arrays):
    return [pltpu.with_memory_space_constraint(v, pltpu.VMEM) for v in arrays]


def swap(value, axis, size, offset):
    return lax.ppermute(value, axis, [(i, i ^ offset) for i in range(size)])


def call(body, out_shape, in_specs, out_specs, scratch=(), vmem=4):
    return pl.pallas_call(
        body,
        out_shape=out_shape,
        in_specs=in_specs,
        out_specs=out_specs,
        scratch_shapes=list(scratch),
        compiler_params=pltpu.CompilerParams(vmem_limit_bytes=vmem << 20),
    )


def take_slots(ids, mask_t, data_rows, pieces, coded):
    block_count, n_mp = mask_t.shape

    def body(ids_ref, mask_ref, rows_ref, *refs):
        outs, sems = refs[:-1], refs[-1]

        def code_of(k):
            shard = ids_ref[0] ^ k
            code = mask_ref[0, shard]
            for b in range(1, block_count):
                code = code + (b + 1) * mask_ref[b, shard]
            return code

        copies = []
        for i, (k, first, count) in enumerate(pieces):
            start = jnp.maximum(code_of(k) - 1, 0) * BLOCK
            src = rows_ref.at[pl.ds(pl.multiple_of(start, BLOCK), BLOCK), pl.ds(first, count)]
            copies.append(pltpu.make_async_copy(src, outs[i], sems.at[i]))
            copies[-1].start()
        for i, k in enumerate(coded):
            outs[-1][i : i + 1, :] = jnp.full((1, LANES), code_of(k), jnp.int32).astype(F32)
        for copy in copies:
            copy.wait()

    shapes = [pltpu.VMEM((BLOCK, count), data_rows.dtype) for _, _, count in pieces]
    if coded:
        shapes.append(jax.ShapeDtypeStruct((n_mp, LANES), F32))
    return call(
        body, shapes, [SMEM, SMEM, ANY], [VMEM] * len(shapes), [pltpu.SemaphoreType.DMA((len(pieces),))], 8
    )(ids, mask_t, *hbm(data_rows))


def load_centroids(centroids, n_parts):
    width, feat = centroids.shape
    part = width // n_parts

    def body(in_ref, out_ref, norm_ref):
        values = in_ref[...]
        out_ref[...] = values
        norm_ref[...] = jnp.sum(jnp.square(values.astype(F32)), axis=1, keepdims=True)

    return pl.pallas_call(
        body,
        out_shape=[pltpu.VMEM((width, feat), centroids.dtype), jax.ShapeDtypeStruct((width, 1), F32)],
        grid=(n_parts,),
        in_specs=[pl.BlockSpec((part, feat), lambda i: (i, 0))],
        out_specs=[pl.BlockSpec((part, feat), lambda i: (i, 0)), pl.BlockSpec((part, 1), lambda i: (i, 0))],
        name="load_centroids",
        compiler_params=pltpu.CompilerParams(vmem_limit_bytes=10 << 20),
    )(*hbm(centroids))


def product(cents_ref, rows_ref):
    return lax.dot_general(
        cents_ref[...], rows_ref[...], (((1,), (1,)), ((), ())), preferred_element_type=F32
    )


def keep(row_refs, pieces, out_ref):
    for ref, (place, first, count) in zip(row_refs, pieces):
        out_ref[place * BLOCK : (place + 1) * BLOCK, first : first + count] = ref[...]


def own_scores(ids, centroids, cent_norm, rows, pieces, state, at, n_slots, n_parts, sharpness):
    width, feat = centroids.shape
    part = width // n_parts
    n_rows = n_slots * BLOCK
    fresh = isinstance(state[0], jax.ShapeDtypeStruct)
    n_in = len(rows)

    def body(ids_ref, cents_ref, norm_ref, *refs):
        row_refs = refs[:n_in]
        rows_out, score_out, lse_out, top_ref, mass_ref = refs[len(refs) - 5 :]
        step = pl.program_id(0)

        @pl.when(step == 0)
        def _():
            keep(row_refs, pieces, rows_out)
            top_ref[...] = jnp.full(top_ref.shape, -NEVER, F32)
            mass_ref[...] = jnp.zeros(mass_ref.shape, F32)

        score = sharpness * (2.0 * product(cents_ref, rows_out) - norm_ref[...])

        @pl.when(step == ids_ref[1])
        def _():
            score_out[...] = score

        old_top = top_ref[...]
        top = jnp.maximum(old_top, jnp.max(score, axis=0, keepdims=True))
        mass = mass_ref[...] * jnp.exp(old_top - top) + jnp.sum(jnp.exp(score - top), axis=0, keepdims=True)
        top_ref[...] = top
        mass_ref[...] = mass
        lse = top + jnp.log(mass)
        for i in range(n_slots):
            lse_out[i] = lse[:, i * BLOCK : (i + 1) * BLOCK]

    grid_spec = pltpu.PrefetchScalarGridSpec(
        num_scalar_prefetch=1,
        grid=(n_parts,),
        in_specs=[
            pl.BlockSpec((part, feat), lambda i, ids: (i, 0)),
            pl.BlockSpec((part, 1), lambda i, ids: (i, 0)),
        ]
        + [pl.BlockSpec(r.shape, lambda i, ids: (0, 0)) for r in rows]
        + ([] if fresh else [ANY] * 3),
        out_specs=[
            pl.BlockSpec((n_rows, feat), lambda i, ids: (at, 0)),
            pl.BlockSpec((part, n_rows), lambda i, ids: (0, at)),
            pl.BlockSpec((n_slots, 1, BLOCK), lambda i, ids: (at, 0, 0)),
        ],
        scratch_shapes=[pltpu.VMEM((1, n_rows), F32)] * 2,
    )
    return pl.pallas_call(
        body,
        out_shape=[pltpu.VMEM(v.shape, v.dtype) for v in state],
        grid_spec=grid_spec,
        input_output_aliases={} if fresh else {3 + n_in + i: i for i in range(3)},
        name="own_scores",
        compiler_params=pltpu.CompilerParams(vmem_limit_bytes=10 << 20),
    )(ids, *vmem(centroids), cent_norm, *rows, *([] if fresh else state))


def first_product(centroids, rows, n_parts):
    width = centroids.shape[0]
    columns = rows.shape[1]
    part = width // n_parts

    def body(cents_ref, rows_ref, out_ref):
        out_ref[...] = product(cents_ref, rows_ref)

    return pl.pallas_call(
        body,
        out_shape=pltpu.VMEM((width, BLOCK), F32),
        grid=(n_parts,),
        in_specs=[
            pl.BlockSpec((part, columns), lambda i: (i, 0)),
            pl.BlockSpec((BLOCK, columns), lambda i: (0, 0)),
        ],
        out_specs=pl.BlockSpec((part, BLOCK), lambda i: (i, 0)),
        name="first_product",
        compiler_params=pltpu.CompilerParams(vmem_limit_bytes=8 << 20),
    )(*vmem(centroids), rows)


def last_scores(ids, centroids, cent_norm, rows, ahead, codes, state, n_parts, sharpness):
    width, feat = centroids.shape
    part = width // n_parts
    wide = 2 * part
    mid = feat // 2
    n_mp = codes.shape[0]
    last = n_mp - 1

    def body(ids_ref, cents_ref, norm_ref, a_ref, b_ref, ahead_ref, code_ref, lse_ref, *refs):
        rows_out, score_out, note_ref, top_ref, mass_ref = refs[len(refs) - 5 :]
        step = pl.program_id(0)

        @pl.when(step == 0)
        def _():
            rows_out[:, :mid] = a_ref[...]
            rows_out[:, mid:] = b_ref[...]
            top_ref[...] = jnp.full(top_ref.shape, -NEVER, F32)
            mass_ref[...] = jnp.zeros(mass_ref.shape, F32)
            for k in range(last):
                note_ref[k : k + 1, :] = lse_ref[k]
            note_ref[n_mp:, :] = code_ref[...]

        score = sharpness * (2.0 * (ahead_ref[...] + product(cents_ref, b_ref)) - norm_ref[...])

        @pl.when(step == ids_ref[1] // 2)
        def _():
            score_out[...] = jnp.where(ids_ref[1] % 2 == 0, score[:part], score[part:])

        old_top = top_ref[...]
        top = jnp.maximum(old_top, jnp.max(score, axis=0, keepdims=True))
        mass = mass_ref[...] * jnp.exp(old_top - top) + jnp.sum(jnp.exp(score - top), axis=0, keepdims=True)
        top_ref[...] = top
        mass_ref[...] = mass
        note_ref[last : last + 1, :] = top + jnp.log(mass)

    def whole(shape):
        return pl.BlockSpec(shape, lambda i, ids: (0,) * len(shape))

    grid_spec = pltpu.PrefetchScalarGridSpec(
        num_scalar_prefetch=1,
        grid=(n_parts // 2,),
        in_specs=[
            pl.BlockSpec((wide, mid), lambda i, ids: (i, 1)),
            pl.BlockSpec((wide, 1), lambda i, ids: (i, 0)),
            whole((BLOCK, mid)),
            whole((BLOCK, mid)),
            pl.BlockSpec((wide, BLOCK), lambda i, ids: (i, 0)),
            whole(codes.shape),
            whole(state[2].shape),
            ANY,
            ANY,
        ],
        out_specs=[
            pl.BlockSpec((BLOCK, feat), lambda i, ids: (last, 0)),
            pl.BlockSpec((part, BLOCK), lambda i, ids: (0, last)),
            whole((2 * n_mp, LANES)),
        ],
        scratch_shapes=[pltpu.VMEM((1, BLOCK), F32)] * 2,
    )
    return pl.pallas_call(
        body,
        out_shape=[pltpu.VMEM(v.shape, v.dtype) for v in state[:2]]
        + [jax.ShapeDtypeStruct((2 * n_mp, LANES), F32)],
        grid_spec=grid_spec,
        input_output_aliases={8: 0, 9: 1},
        name="last_scores",
        compiler_params=pltpu.CompilerParams(vmem_limit_bytes=10 << 20),
    )(ids, *vmem(centroids), cent_norm, *rows, ahead, codes, state[2], *state[:2])


def side_scores(ids, centroids, cent_norm, sides, pieces, state, at, n_slots, half, sharpness):
    feat = centroids.shape[1]
    n_rows = n_slots * BLOCK
    fresh = isinstance(state[0], jax.ShapeDtypeStruct)
    n_in = len(sides[0])

    def body(ids_ref, cents_ref, norm_ref, *refs):
        x_refs, y_refs = refs[:n_in], refs[n_in : 2 * n_in]
        x_rows, y_rows, x_out, y_out = refs[len(refs) - 4 :]
        step = pl.program_id(0)

        def score(rows_ref):
            return sharpness * (2.0 * product(cents_ref, rows_ref) - norm_ref[...])

        @pl.when(step == 0)
        def _():
            keep(x_refs, pieces, x_rows)
            keep(y_refs, pieces, y_rows)

        @pl.when(step != 3)
        def _():
            x_out[...] = score(x_rows)

        @pl.when(step != 2)
        def _():
            y_out[...] = score(y_rows)

    def block(i, ids):
        mine = ids[1]
        other = jnp.where(i == 2, 2 * (mine ^ 2) + 1, 2 * (mine ^ 1))
        return (jnp.where(i < 2, 2 * mine + i, other), 0)

    grid_spec = pltpu.PrefetchScalarGridSpec(
        num_scalar_prefetch=1,
        grid=(4,),
        in_specs=[pl.BlockSpec((half, feat), block), pl.BlockSpec((half, 1), block)]
        + [pl.BlockSpec(r.shape, lambda i, ids: (0, 0)) for r in sides[0] + sides[1]]
        + ([] if fresh else [ANY] * 4),
        out_specs=[
            pl.BlockSpec((n_rows, feat), lambda i, ids: (at, 0)),
            pl.BlockSpec((n_rows, feat), lambda i, ids: (at, 0)),
            pl.BlockSpec((half, n_rows), lambda i, ids: (jnp.minimum(i, 2), at)),
            pl.BlockSpec((half, n_rows), lambda i, ids: (jnp.where(i == 3, 2, jnp.minimum(i, 1)), at)),
        ],
    )
    return pl.pallas_call(
        body,
        out_shape=[pltpu.VMEM(v.shape, v.dtype) for v in state],
        grid_spec=grid_spec,
        input_output_aliases={} if fresh else {3 + 2 * n_in + i: i for i in range(4)},
        name="side_scores",
        compiler_params=pltpu.CompilerParams(vmem_limit_bytes=12 << 20),
    )(ids, *vmem(centroids), cent_norm, *sides[0], *sides[1], *([] if fresh else state))


def one_side_scores(ids, centroids, cent_norm, rows, pieces, state, at, n_slots, half, sharpness, bit):
    feat = centroids.shape[1]
    n_rows = n_slots * BLOCK
    n_in = len(rows)

    def body(ids_ref, cents_ref, norm_ref, *refs):
        rows_out, score_out = refs[len(refs) - 2 :]

        @pl.when(pl.program_id(0) == 0)
        def _():
            keep(refs[:n_in], pieces, rows_out)

        score_out[...] = sharpness * (2.0 * product(cents_ref, rows_out) - norm_ref[...])

    def block(i, ids):
        mine = ids[1]
        other = 2 * (mine ^ 2) + 1 if bit == 1 else 2 * (mine ^ 1)
        return (jnp.where(i < 2, 2 * mine + i, other), 0)

    grid_spec = pltpu.PrefetchScalarGridSpec(
        num_scalar_prefetch=1,
        grid=(3,),
        in_specs=[pl.BlockSpec((half, feat), block), pl.BlockSpec((half, 1), block)]
        + [pl.BlockSpec(r.shape, lambda i, ids: (0, 0)) for r in rows]
        + [ANY] * 2,
        out_specs=[
            pl.BlockSpec((n_rows, feat), lambda i, ids: (at, 0)),
            pl.BlockSpec((half, n_rows), lambda i, ids: (i, at)),
        ],
    )
    return pl.pallas_call(
        body,
        out_shape=[pltpu.VMEM(v.shape, v.dtype) for v in state],
        grid_spec=grid_spec,
        input_output_aliases={3 + n_in + i: i for i in range(2)},
        name="one_side_scores",
        compiler_params=pltpu.CompilerParams(vmem_limit_bytes=12 << 20),
    )(ids, *vmem(centroids), cent_norm, *rows, *state)


def log_total(kept):
    peak = jnp.maximum(jnp.max(kept, axis=0, keepdims=True), 0.0)
    mass = jnp.sum(jnp.exp(kept - peak), axis=0, keepdims=True)
    return peak + jnp.log(jnp.exp(-peak) + mass)


def combine(notes, seq, block_count):
    n_mp = 2 * len(notes)

    def body(*refs):
        note_refs, (slot_ref, row_ref) = refs[: len(notes)], refs[len(notes) :]

        def rows(j, first, count):
            start = 2 * n_mp * (j % 2) + first
            return note_refs[j // 2][start : start + count, :]

        for i, k in enumerate(seq):
            lse = jnp.concatenate([rows(k ^ j, at, 1) for at, j in enumerate(seq)], axis=0)
            code = rows(k, n_mp, n_mp)
            mine = code[i : i + 1, :]
            total = log_total(jnp.where((code == mine) & (code > 0.0), lse, -NEVER))
            slot_ref[i : i + 1, :] = jnp.where(mine > 0.0, total, NEVER)
            if k == 0:
                for b in range(block_count):
                    row_ref[b : b + 1, :] = log_total(jnp.where(code == float(b + 1), lse, -NEVER))

    return call(
        body,
        [jax.ShapeDtypeStruct((n_mp, LANES), F32), jax.ShapeDtypeStruct((block_count, LANES), F32)],
        [VMEM] * len(notes),
        [VMEM, VMEM],
    )(*notes)


def weights_of(score_ref, norm_ref, into, column, total):
    for k in range(norm_ref.shape[0]):
        tile = jnp.exp(score_ref[:, k * BLOCK : (k + 1) * BLOCK] - norm_ref[k : k + 1, :])
        total = tile if total is None else total + tile
        into[:, column + k * BLOCK : column + (k + 1) * BLOCK] = tile.astype(BF16)
    return total


def sent_sums(side_rows, side_score, norms, half, first, columns, tile, with_counts):
    n_rows = side_rows[0].shape[0]
    steps = columns // tile

    def body(x_ref, y_ref, xs_ref, ys_ref, xn_ref, yn_ref, x_out, y_out, w_buf, c_buf):
        step = pl.program_id(0)

        @pl.when(step == 0)
        def _():
            for i, (s_ref, n_ref) in enumerate(((xs_ref, xn_ref), (ys_ref, yn_ref))):
                total = weights_of(s_ref, n_ref, w_buf.at[i], 0, None)
                c_buf[i] = jnp.broadcast_to(jnp.sum(total, axis=1, keepdims=True), c_buf.shape[1:])

        for i, (r_ref, out) in enumerate(((x_ref, x_out), (y_ref, y_out))):
            counts = c_buf[i]

            @pl.when(step < steps)
            def _():
                part = jnp.dot(w_buf[i], r_ref[...], preferred_element_type=F32)
                out[...] = part * (2.0**10 / jnp.maximum(counts[:, 0:1], 2.0**-20))

            @pl.when(step == steps)
            def _():
                hi = counts.astype(BF16).astype(F32)
                mid = (counts - hi).astype(BF16).astype(F32)
                low = (counts - hi - mid).astype(BF16).astype(F32)
                lane = lax.broadcasted_iota(jnp.int32, counts.shape, 1)
                terms = jnp.where(lane == 0, hi, jnp.where(lane == 1, mid, jnp.where(lane == 2, low, 0.0)))
                out[:, :LANES] = terms

    base = first // tile
    rows_spec = pl.BlockSpec((n_rows, tile), lambda i: (0, base + jnp.minimum(i, steps - 1)))
    score_spec = pl.BlockSpec((half, n_rows), lambda i: (2, 0))
    norm_spec = pl.BlockSpec(norms[0].shape, lambda i: (0, 0))
    out_spec = pl.BlockSpec((half, tile), lambda i: (0, i))
    width = columns + LANES if with_counts else columns
    return pl.pallas_call(
        body,
        out_shape=[jax.ShapeDtypeStruct((half, width), F32)] * 2,
        grid=(steps + 1 if with_counts else steps,),
        in_specs=[rows_spec] * 2 + [score_spec] * 2 + [norm_spec] * 2,
        out_specs=[out_spec] * 2,
        scratch_shapes=[pltpu.VMEM((2, half, n_rows), BF16), pltpu.VMEM((2, half, LANES), F32)],
        name="sent_sums",
        compiler_params=pltpu.CompilerParams(vmem_limit_bytes=16 << 20),
    )(*vmem(*side_rows, *side_score), *norms)


def own_sums(ids, rows, scores, norms, parts, centroids, width, tile, done):
    n_rows, feat = rows[0].shape
    half = width // 2

    def body(ids_ref, *refs):
        row_refs, score_refs, norm_refs = refs[:3], refs[3:6], refs[6:9]
        part_refs, tail_refs, old_ref = refs[9:11], refs[11:13], refs[13]
        out_ref, count_ref, new_ref, sent_ref, square_ref, w_buf = refs[14:]

        @pl.when(pl.program_id(0) == 0)
        def _():
            total = None
            for i in range(3):
                total = weights_of(score_refs[i], norm_refs[i], w_buf, i * n_rows, total)
            count_ref[...] = jnp.sum(total, axis=1, keepdims=True)

        acc = jnp.dot(w_buf[:, :n_rows], row_refs[0][...], preferred_element_type=F32)
        acc += jnp.dot(w_buf[:, n_rows : 2 * n_rows], row_refs[1][...], preferred_element_type=F32)
        acc += jnp.dot(w_buf[:, 2 * n_rows :], row_refs[2][...], preferred_element_type=F32)
        out_ref[...] = acc

        @pl.when(pl.program_id(0) == done)
        def _():
            for i in range(2):
                span = slice(i * half, (i + 1) * half)
                lane = lax.broadcasted_iota(jnp.int32, (half, LANES), 1)
                sent = jnp.sum(jnp.where(lane < 3, tail_refs[i][...], 0.0), axis=1, keepdims=True)
                back = part_refs[i][...] * (jnp.maximum(sent, 2.0**-20) * 2.0**-10)
                before = old_ref[span, :].astype(F32)
                after = (out_ref[span, :] + back + before) / (count_ref[span, :] + sent + 1.0)
                new_ref[span, :] = after
                sent_ref[span, :] = sent
                square_ref[span, :] = jnp.sum(jnp.square(after - before), axis=1, keepdims=True)

    def whole(shape):
        return pl.BlockSpec(shape, lambda i, ids: (0,) * len(shape))

    thin = jax.ShapeDtypeStruct((width, 1), F32)
    return pl.pallas_call(
        body,
        out_shape=[
            pltpu.VMEM((width, feat), F32),
            thin,
            jax.ShapeDtypeStruct((width, feat), F32),
            thin,
            thin,
        ],
        grid_spec=pltpu.PrefetchScalarGridSpec(
            num_scalar_prefetch=1,
            grid=(feat // tile,),
            in_specs=[pl.BlockSpec((n_rows, tile), lambda i, ids: (0, i))] * 3
            + [whole((width, n_rows))] * 3
            + [whole(norms[0].shape)] * 3
            + [whole((half, tile))] * 2
            + [pl.BlockSpec((half, LANES), lambda i, ids: (0, tile // LANES))] * 2
            + [pl.BlockSpec((width, tile), lambda i, ids: (ids[1], done))],
            out_specs=[
                pl.BlockSpec((width, tile), lambda i, ids: (0, i)),
                whole((width, 1)),
                pl.BlockSpec((width, tile), lambda i, ids: (0, done)),
                whole((width, 1)),
                whole((width, 1)),
            ],
            scratch_shapes=[pltpu.VMEM((width, 3 * n_rows), BF16)],
        ),
        name="own_sums",
        compiler_params=pltpu.CompilerParams(vmem_limit_bytes=24 << 20),
    )(ids, *vmem(*rows, *scores), *norms, *parts, *parts, *vmem(centroids))


def update(ids, own, counts, parts, centroids, first, columns, state, final, n_devices):
    width, feat = own.shape
    half = width // 2
    at = first // columns

    def body(ids_ref, own_ref, count_ref, a_ref, b_ref, old_ref, sent_in, square_in, _, new_ref, *refs):
        i = pl.program_id(0)

        def finish(part_ref):
            sent = sent_in[...]
            back = part_ref[...] * (jnp.maximum(sent, 2.0**-20) * 2.0**-10)
            before = old_ref[...].astype(F32)
            after = (own_ref[...] + back + before) / (count_ref[...] + sent + 1.0)
            new_ref[...] = after
            total = square_in[...] + jnp.sum(jnp.square(after - before), axis=1, keepdims=True)
            if not final:
                refs[0][...] = total
                return
            move_ref, peak_ref = refs
            move = jnp.sqrt(total + 1.0)
            move_ref[...] = move
            top = jnp.broadcast_to(jnp.max(move, axis=0, keepdims=True), peak_ref.shape)
            peak_ref[...] = jnp.where(i == 0, top, jnp.maximum(top, peak_ref[...]))

        @pl.when(i == 0)
        def _():
            finish(a_ref)

        @pl.when(i == 1)
        def _():
            finish(b_ref)

    column = pl.BlockSpec((half, 1), lambda i, ids: (i, 0))
    block = pl.BlockSpec((half, columns), lambda i, ids: (i, at))
    thin = jax.ShapeDtypeStruct((width, 1), F32)
    new, sent, square = state
    out_shape = [jax.ShapeDtypeStruct((width, feat), F32), thin]
    out_specs = [block, column]
    if final:
        out_shape.append(jax.ShapeDtypeStruct((n_devices, LANES), F32))
        out_specs.append(pl.BlockSpec((n_devices, LANES), lambda i, ids: (0, 0)))
    return pl.pallas_call(
        body,
        out_shape=out_shape,
        grid_spec=pltpu.PrefetchScalarGridSpec(
            num_scalar_prefetch=1,
            grid=(2,),
            in_specs=[
                block,
                column,
                pl.BlockSpec((half, columns), lambda i, ids: (0, 0)),
                pl.BlockSpec((half, columns), lambda i, ids: (0, 0)),
                pl.BlockSpec((half, columns), lambda i, ids: (2 * ids[1] + i, at)),
                column,
                column,
                ANY,
            ],
            out_specs=out_specs,
        ),
        input_output_aliases={8: 0},
        name="update",
        compiler_params=pltpu.CompilerParams(vmem_limit_bytes=10 << 20),
    )(ids, *vmem(own), counts, *parts, *vmem(centroids), sent, square, new)


def sequence(n_mp):
    return [0, 1, 6, 2, 3, 7, 4, 5] if n_mp == 8 else list(range(n_mp))


def pieces_of(n_mp, feat):
    mid = feat // 2
    seq = sequence(n_mp)
    return [[(k, 0, feat)] if at < n_mp - 3 else [(k, 0, mid), (k, mid, mid)] for at, k in enumerate(seq)]


def own_groups(n_mp):
    return [(k, k + 1) for k in range(0, n_mp - 2, 2)] + [(n_mp - 2,)]


def on_square(data_rows, centroids, block_mask, lower_bound):
    feat = data_rows.shape[1]
    width = centroids.shape[0]
    block_count = data_rows.shape[0] // BLOCK
    n_mp = lax.axis_size("mp")
    n_dp = lax.axis_size("dp")
    own_width = width // n_dp
    half = own_width // 2
    my_mp = lax.axis_index("mp").astype(jnp.int32)
    my_dp = lax.axis_index("dp").astype(jnp.int32)
    sharpness = 4.0 / math.sqrt(feat)
    ids = jnp.stack([my_mp, my_dp])
    mask_t = block_mask.T

    seq = sequence(n_mp)
    last = seq[-1]
    cuts = {cut[0][0]: cut for cut in pieces_of(n_mp, feat)}
    early = [p for k in seq[2:5] for p in cuts[k]]
    late = cuts[0] + [p for k in seq[5:] for p in cuts[k]] + cuts[1]
    got = dict(zip(early, take_slots(ids, mask_t, data_rows, early, [])))
    *rest, codes = take_slots(ids, mask_t, data_rows, late, seq)
    got.update(zip(late, rest))
    for piece in early + late[1:]:
        got[piece] = swap(got[piece], "mp", n_mp, piece[0])

    side = {}
    for k in seq:
        for piece in cuts[k]:
            for bit in (1, 2):
                side[bit, piece] = swap(got[piece], "dp", n_dp, bit)

    cents, cent_norm = load_centroids(centroids, 2 * n_dp)

    n_rows = n_mp * BLOCK
    own = [
        jax.ShapeDtypeStruct((n_rows, feat), BF16),
        jax.ShapeDtypeStruct((own_width, n_rows), F32),
        jax.ShapeDtypeStruct((n_mp, 1, BLOCK), F32),
    ]
    sides = [jax.ShapeDtypeStruct((n_rows, feat), BF16)] * 2
    sides += [jax.ShapeDtypeStruct((3 * half, n_rows), F32)] * 2
    ahead = first_product(cents, got[cuts[last][0]], n_dp)
    for group in own_groups(n_mp):
        held = [p for at in group for p in cuts[seq[at]]]
        placed = [(seq.index(p[0]) - group[0], p[1], p[2]) for p in held]
        own = own_scores(
            ids, cents, cent_norm, [got[p] for p in held], placed, own, group[0] // len(group), len(group),
            n_dp, sharpness,
        )
    for i in range(n_mp // 2):
        held = cuts[seq[2 * i]] + cuts[seq[2 * i + 1]]
        placed = [(seq.index(p[0]) - 2 * i, p[1], p[2]) for p in held]
        pair = [[side[bit, p] for p in held] for bit in (1, 2)]
        if i < n_mp // 2 - 1:
            sides = list(side_scores(ids, cents, cent_norm, pair, placed, sides, i, 2, half, sharpness))
            continue
        for bit in (1, 2):
            sides[bit - 1 :: 2] = one_side_scores(
                ids, cents, cent_norm, pair[bit - 1], placed, sides[bit - 1 :: 2], i, 2, half, sharpness, bit
            )

    *own, note = last_scores(ids, cents, cent_norm, [got[p] for p in cuts[last]], ahead, codes, own, n_dp, sharpness)
    beside = swap(note, "mp", n_mp, 1)
    both = jnp.concatenate([note, beside])
    notes = [both]
    for k in range(2, n_mp, 2):
        notes.append(swap(both, "mp", n_mp, k))
    slot_norm, row_norm = combine(notes, seq, block_count)
    log_norm = row_norm.reshape(-1)
    side_norm = []
    for bit in (1, 2):
        side_norm.append(swap(slot_norm, "dp", n_dp, bit))

    tile = feat // 4
    spans = [(3 * tile, tile), (0, 2 * tile), (2 * tile, tile)]
    received = []
    for i, (first, columns) in enumerate(spans):
        sent = sent_sums(sides[:2], sides[2:], side_norm, half, first, columns, tile, i == 0)
        for_y, for_x = [v.astype(jnp.float16) for v in sent]
        pair = []
        for bit, message in ((1, for_x), (2, for_y)):
            pair.append(swap(message, "dp", n_dp, bit).astype(F32))
        received.append(pair)
    total, counts, updated, sent, square = own_sums(
        ids,
        [own[0], sides[0], sides[1]],
        [own[1], sides[2], sides[3]],
        [slot_norm] + side_norm,
        received[0],
        cents,
        own_width,
        tile,
        spans[0][0] // tile,
    )
    for i, (first, columns) in list(enumerate(spans))[1:]:
        updated, square, *peak = update(
            ids, total, counts, received[i], cents, first, columns, [updated, sent, square], i == 2, n_dp * n_mp
        )
    movement, peak = square, peak[0]
    shard_peaks = lax.all_to_all(peak, ("dp", "mp"), split_axis=0, concat_axis=0, tiled=True)
    shard_peak = jnp.max(shard_peaks.reshape(n_dp, n_mp, LANES), axis=(0, 2))
    new_lower = lower_bound - shard_peak[:, None]
    return (updated, movement[:, 0], log_norm, new_lower)


def on_device(data_rows, centroids, block_mask, lower_bound):
    feat = data_rows.shape[1]
    width = centroids.shape[0]
    block_count = data_rows.shape[0] // BLOCK
    n_mp = lax.axis_size("mp")
    n_dp = lax.axis_size("dp")
    own_width = width // n_dp
    my_mp = lax.axis_index("mp")
    my_dp = lax.axis_index("dp")
    sharpness = 4.0 / math.sqrt(feat)

    labels = jnp.arange(1, block_count + 1, dtype=jnp.int32)
    codes = jnp.sum(block_mask * labels[None, :], axis=1)

    def outgoing(k):
        code = lax.dynamic_index_in_dim(codes, my_mp ^ k, 0, keepdims=False)
        start = jnp.maximum(code - 1, 0) * BLOCK
        return lax.dynamic_slice(data_rows, (start, 0), (BLOCK, feat))

    order = list(range(2, n_mp)) + [1]
    got = {0: outgoing(0)}
    for k in order:
        got[k] = swap(outgoing(k), "mp", n_mp, k)

    cent_norm = jnp.sum(jnp.square(centroids.astype(jnp.float32)), axis=1)

    scores, lses = {}, {}
    groups = [(k, k + 1) for k in range(0, n_mp, 2)]
    for group in groups:
        rows = jnp.concatenate([got[k] for k in group], axis=0)
        product = lax.dot_general(
            centroids, rows, (((1,), (1,)), ((), ())), preferred_element_type=jnp.float32
        )
        score = sharpness * (2.0 * product - cent_norm[:, None])
        top = jnp.max(score, axis=0)
        lse = top + jnp.log(jnp.sum(jnp.exp(score - top[None, :]), axis=0))
        scores[group] = score
        for i, k in enumerate(group):
            lses[k] = lse[i * BLOCK : (i + 1) * BLOCK]

    note = jnp.concatenate(
        [
            jnp.stack([lses[k] for k in range(n_mp)]),
            jnp.pad(codes.astype(jnp.float32), (0, BLOCK - n_mp))[None, :],
        ]
    )
    notes = lax.all_to_all(
        jnp.broadcast_to(note[None], (n_mp,) + note.shape), "mp", split_axis=0, concat_axis=0, tiled=True
    )
    shard_ids = jnp.arange(n_mp, dtype=jnp.int32)
    lse_of = notes[:, :n_mp, :]
    all_code = notes[:, n_mp, :n_mp].astype(jnp.int32)
    all_lse = lse_of[shard_ids[None, :], shard_ids[None, :] ^ shard_ids[:, None]]
    tops = jnp.where((all_code > 0)[:, :, None], all_lse, -1e30)

    def normalizer(same, lse):
        kept = jnp.where(same[:, :, None], lse, -1e30)
        peak = jnp.maximum(jnp.max(kept, axis=1), 0.0)
        mass = jnp.sum(jnp.exp(kept - peak[:, None, :]), axis=1)
        return peak + jnp.log(jnp.exp(-peak) + mass)

    my_lse = lax.dynamic_index_in_dim(tops, my_mp, 0, keepdims=False)
    row_norm = normalizer(codes[None, :] == labels[:, None], jnp.broadcast_to(my_lse[None], (block_count,) + my_lse.shape))
    log_norm = row_norm.reshape(-1)

    slot_code = lax.dynamic_index_in_dim(all_code, my_mp, 1, keepdims=False)
    slot_norm = normalizer((all_code == slot_code[:, None]) & (all_code > 0), tops)

    weights, counts = [], 0.0
    for group in groups:
        src = [my_mp ^ k for k in group]
        norm = jnp.concatenate([slot_norm[m] for m in src])
        valid = jnp.concatenate([jnp.broadcast_to(slot_code[m] > 0, (BLOCK,)) for m in src])
        weight = jnp.where(valid[None, :], jnp.exp(scores[group] - norm[None, :]), 0.0)
        counts = counts + jnp.sum(weight, axis=1)
        weights.append(weight.astype(jnp.bfloat16))
    weight_half = jnp.concatenate(weights, axis=1)
    rows = jnp.concatenate([got[k] for k in range(n_mp)], axis=0)

    def quarter(j):
        return (my_dp ^ j) * own_width

    def partial(j, half):
        w = lax.dynamic_slice(weight_half, (quarter(j), 0), (own_width, weight_half.shape[1]))
        x = lax.slice_in_dim(rows, half * (feat // 2), (half + 1) * (feat // 2), axis=1)
        return lax.dot_general(w, x, (((1,), (0,)), ((), ())), preferred_element_type=jnp.float32)

    count_of = {0: counts}
    for j in range(1, n_dp):
        count_of[j] = swap(counts, "dp", n_dp, j)

    def sub(vec, j):
        return lax.dynamic_slice(vec, (quarter(j),), (own_width,))

    def scale(members, j):
        total = sum(sub(count_of[i], j) for i in members)
        return jnp.maximum(total, 2.0**-20)[:, None] * 2.0**-10

    bits = [1 << b for b in range(n_dp.bit_length() - 1)]
    plan = [bits, bits[::-1]]
    current = [{}, {}]
    for j in reversed(range(n_dp)):
        for half in range(2):
            jj = j if half == 0 or n_dp != 4 else {3: 3, 1: 2, 2: 1, 0: 0}[j]
            current[half][jj] = None
    todo = [[j for j in reversed(range(n_dp))] for _ in range(2)]
    for half in range(2):
        for j in todo[half]:
            current[half][j] = partial(j, half)
    members = [{0}, {0}]
    for step in range(len(bits)):
        for half in range(2):
            bit = plan[half][step]
            cur = current[half]
            mine = members[half]
            theirs = {i ^ bit for i in mine}
            kept = {}
            for j in sorted(cur, reverse=True):
                if not j & bit:
                    continue
                sent = (cur[j] / scale(mine, j)).astype(jnp.float16)
                back = swap(sent, "dp", n_dp, bit)
                kept[j ^ bit] = cur[j ^ bit] + back.astype(jnp.float32) * scale(theirs, j ^ bit)
            current[half] = kept
            members[half] = mine | theirs
    part_sums = jnp.concatenate([current[0][0], current[1][0]], axis=1)
    part_counts = sum(sub(count_of[j], 0) for j in range(n_dp))

    old_cents = lax.dynamic_slice_in_dim(centroids, my_dp * own_width, own_width, 0).astype(jnp.float32)
    updated = (part_sums + old_cents) / (part_counts[:, None] + 1.0)
    movement = jnp.sqrt(jnp.sum(jnp.square(updated - old_cents), axis=1) + 1.0)
    peak = jnp.broadcast_to(jnp.max(movement), (n_dp * n_mp, 1))
    shard_peaks = lax.all_to_all(peak, ("dp", "mp"), split_axis=0, concat_axis=0, tiled=True)
    shard_peak = jnp.max(shard_peaks.reshape(n_dp, n_mp), axis=0)
    new_lower = lower_bound - shard_peak[:, None]
    return (updated, movement, log_norm, new_lower)


def solution(mesh):
    placed = (P(("dp", "mp"), None), P("mp", None), P(None, ("dp", "mp")), P(None, ("dp", "mp")))
    square = mesh.shape["dp"] == 4

    def body(*args):
        return on_square(*args) if square else on_device(*args)

    return jax.shard_map(
        body,
        mesh=mesh,
        in_specs=placed,
        out_specs=(P(("mp", "dp"), None), P(("mp", "dp")), P(("dp", "mp")), P(None, ("dp", "mp"))),
        check_vma=False,
    )
```

```python
import math

import jax
import jax.numpy as jnp
from jax import lax
from jax.experimental import pallas as pl
from jax.experimental.pallas import tpu as pltpu
from jax.sharding import PartitionSpec as P


BLOCK = 128
LANES = 128
F32 = jnp.float32
BF16 = jnp.bfloat16
NEVER = 1e30
ANY = pl.BlockSpec(memory_space=pl.ANY)
SMEM = pl.BlockSpec(memory_space=pltpu.SMEM)
VMEM = pl.BlockSpec(memory_space=pltpu.VMEM)


def hbm(*arrays):
    return [pltpu.with_memory_space_constraint(v, pltpu.HBM) for v in arrays]


def vmem(*arrays):
    return [pltpu.with_memory_space_constraint(v, pltpu.VMEM) for v in arrays]


def swap(value, axis, size, offset):
    return lax.ppermute(value, axis, [(i, i ^ offset) for i in range(size)])


def call(body, out_shape, in_specs, out_specs, scratch=(), vmem=4):
    return pl.pallas_call(
        body,
        out_shape=out_shape,
        in_specs=in_specs,
        out_specs=out_specs,
        scratch_shapes=list(scratch),
        compiler_params=pltpu.CompilerParams(vmem_limit_bytes=vmem << 20),
    )


def take_slots(ids, mask_t, data_rows, pieces, coded):
    block_count, n_mp = mask_t.shape

    def body(ids_ref, mask_ref, rows_ref, *refs):
        outs, sems = refs[:-1], refs[-1]

        def code_of(k):
            shard = ids_ref[0] ^ k
            code = mask_ref[0, shard]
            for b in range(1, block_count):
                code = code + (b + 1) * mask_ref[b, shard]
            return code

        copies = []
        for i, (k, first, count) in enumerate(pieces):
            start = jnp.maximum(code_of(k) - 1, 0) * BLOCK
            src = rows_ref.at[pl.ds(pl.multiple_of(start, BLOCK), BLOCK), pl.ds(first, count)]
            copies.append(pltpu.make_async_copy(src, outs[i], sems.at[i]))
            copies[-1].start()
        for i, k in enumerate(coded):
            outs[-1][i : i + 1, :] = jnp.full((1, LANES), code_of(k), jnp.int32).astype(F32)
        for copy in copies:
            copy.wait()

    shapes = [pltpu.VMEM((BLOCK, count), data_rows.dtype) for _, _, count in pieces]
    if coded:
        shapes.append(jax.ShapeDtypeStruct((n_mp, LANES), F32))
    return call(
        body, shapes, [SMEM, SMEM, ANY], [VMEM] * len(shapes), [pltpu.SemaphoreType.DMA((len(pieces),))], 8
    )(ids, mask_t, *hbm(data_rows))


def load_centroids(centroids, n_parts):
    width, feat = centroids.shape
    part = width // n_parts

    def body(in_ref, out_ref, norm_ref):
        values = in_ref[...]
        out_ref[...] = values
        norm_ref[...] = jnp.sum(jnp.square(values.astype(F32)), axis=1, keepdims=True)

    return pl.pallas_call(
        body,
        out_shape=[pltpu.VMEM((width, feat), centroids.dtype), jax.ShapeDtypeStruct((width, 1), F32)],
        grid=(n_parts,),
        in_specs=[pl.BlockSpec((part, feat), lambda i: (i, 0))],
        out_specs=[pl.BlockSpec((part, feat), lambda i: (i, 0)), pl.BlockSpec((part, 1), lambda i: (i, 0))],
        name="load_centroids",
        compiler_params=pltpu.CompilerParams(vmem_limit_bytes=10 << 20),
    )(*hbm(centroids))


def product(cents_ref, rows_ref):
    return lax.dot_general(
        cents_ref[...], rows_ref[...], (((1,), (1,)), ((), ())), preferred_element_type=F32
    )


def keep(row_refs, pieces, out_ref):
    for ref, (place, first, count) in zip(row_refs, pieces):
        out_ref[place * BLOCK : (place + 1) * BLOCK, first : first + count] = ref[...]


def own_scores(ids, centroids, cent_norm, rows, pieces, state, at, n_slots, n_parts, sharpness):
    width, feat = centroids.shape
    part = width // n_parts
    n_rows = n_slots * BLOCK
    fresh = isinstance(state[0], jax.ShapeDtypeStruct)
    n_in = len(rows)

    def body(ids_ref, cents_ref, norm_ref, *refs):
        row_refs = refs[:n_in]
        rows_out, score_out, lse_out, top_ref, mass_ref = refs[len(refs) - 5 :]
        step = pl.program_id(0)

        @pl.when(step == 0)
        def _():
            keep(row_refs, pieces, rows_out)
            top_ref[...] = jnp.full(top_ref.shape, -NEVER, F32)
            mass_ref[...] = jnp.zeros(mass_ref.shape, F32)

        score = sharpness * (2.0 * product(cents_ref, rows_out) - norm_ref[...])

        @pl.when(step == ids_ref[1])
        def _():
            score_out[...] = score

        old_top = top_ref[...]
        top = jnp.maximum(old_top, jnp.max(score, axis=0, keepdims=True))
        mass = mass_ref[...] * jnp.exp(old_top - top) + jnp.sum(jnp.exp(score - top), axis=0, keepdims=True)
        top_ref[...] = top
        mass_ref[...] = mass
        lse = top + jnp.log(mass)
        for i in range(n_slots):
            lse_out[i] = lse[:, i * BLOCK : (i + 1) * BLOCK]

    grid_spec = pltpu.PrefetchScalarGridSpec(
        num_scalar_prefetch=1,
        grid=(n_parts,),
        in_specs=[
            pl.BlockSpec((part, feat), lambda i, ids: (i, 0)),
            pl.BlockSpec((part, 1), lambda i, ids: (i, 0)),
        ]
        + [pl.BlockSpec(r.shape, lambda i, ids: (0, 0)) for r in rows]
        + ([] if fresh else [ANY] * 3),
        out_specs=[
            pl.BlockSpec((n_rows, feat), lambda i, ids: (at, 0)),
            pl.BlockSpec((part, n_rows), lambda i, ids: (0, at)),
            pl.BlockSpec((n_slots, 1, BLOCK), lambda i, ids: (at, 0, 0)),
        ],
        scratch_shapes=[pltpu.VMEM((1, n_rows), F32)] * 2,
    )
    return pl.pallas_call(
        body,
        out_shape=[pltpu.VMEM(v.shape, v.dtype) for v in state],
        grid_spec=grid_spec,
        input_output_aliases={} if fresh else {3 + n_in + i: i for i in range(3)},
        name="own_scores",
        compiler_params=pltpu.CompilerParams(vmem_limit_bytes=10 << 20),
    )(ids, *vmem(centroids), cent_norm, *rows, *([] if fresh else state))


def first_product(centroids, rows, n_parts):
    width = centroids.shape[0]
    columns = rows.shape[1]
    part = width // n_parts

    def body(cents_ref, rows_ref, out_ref):
        out_ref[...] = product(cents_ref, rows_ref)

    return pl.pallas_call(
        body,
        out_shape=pltpu.VMEM((width, BLOCK), F32),
        grid=(n_parts,),
        in_specs=[
            pl.BlockSpec((part, columns), lambda i: (i, 0)),
            pl.BlockSpec((BLOCK, columns), lambda i: (0, 0)),
        ],
        out_specs=pl.BlockSpec((part, BLOCK), lambda i: (i, 0)),
        name="first_product",
        compiler_params=pltpu.CompilerParams(vmem_limit_bytes=8 << 20),
    )(*vmem(centroids), rows)


def last_scores(ids, centroids, cent_norm, rows, ahead, codes, state, n_parts, sharpness):
    width, feat = centroids.shape
    part = width // n_parts
    wide = 2 * part
    mid = feat // 2
    n_mp = codes.shape[0]
    last = n_mp - 1

    def body(ids_ref, cents_ref, norm_ref, a_ref, b_ref, ahead_ref, code_ref, lse_ref, *refs):
        rows_out, score_out, note_ref, top_ref, mass_ref = refs[len(refs) - 5 :]
        step = pl.program_id(0)

        @pl.when(step == 0)
        def _():
            rows_out[:, :mid] = a_ref[...]
            rows_out[:, mid:] = b_ref[...]
            top_ref[...] = jnp.full(top_ref.shape, -NEVER, F32)
            mass_ref[...] = jnp.zeros(mass_ref.shape, F32)
            for k in range(last):
                note_ref[k : k + 1, :] = lse_ref[k]
            note_ref[n_mp:, :] = code_ref[...]

        score = sharpness * (2.0 * (ahead_ref[...] + product(cents_ref, b_ref)) - norm_ref[...])

        @pl.when(step == ids_ref[1] // 2)
        def _():
            score_out[...] = jnp.where(ids_ref[1] % 2 == 0, score[:part], score[part:])

        old_top = top_ref[...]
        top = jnp.maximum(old_top, jnp.max(score, axis=0, keepdims=True))
        mass = mass_ref[...] * jnp.exp(old_top - top) + jnp.sum(jnp.exp(score - top), axis=0, keepdims=True)
        top_ref[...] = top
        mass_ref[...] = mass
        note_ref[last : last + 1, :] = top + jnp.log(mass)

    def whole(shape):
        return pl.BlockSpec(shape, lambda i, ids: (0,) * len(shape))

    grid_spec = pltpu.PrefetchScalarGridSpec(
        num_scalar_prefetch=1,
        grid=(n_parts // 2,),
        in_specs=[
            pl.BlockSpec((wide, mid), lambda i, ids: (i, 1)),
            pl.BlockSpec((wide, 1), lambda i, ids: (i, 0)),
            whole((BLOCK, mid)),
            whole((BLOCK, mid)),
            pl.BlockSpec((wide, BLOCK), lambda i, ids: (i, 0)),
            whole(codes.shape),
            whole(state[2].shape),
            ANY,
            ANY,
        ],
        out_specs=[
            pl.BlockSpec((BLOCK, feat), lambda i, ids: (last, 0)),
            pl.BlockSpec((part, BLOCK), lambda i, ids: (0, last)),
            whole((2 * n_mp, LANES)),
        ],
        scratch_shapes=[pltpu.VMEM((1, BLOCK), F32)] * 2,
    )
    return pl.pallas_call(
        body,
        out_shape=[pltpu.VMEM(v.shape, v.dtype) for v in state[:2]]
        + [jax.ShapeDtypeStruct((2 * n_mp, LANES), F32)],
        grid_spec=grid_spec,
        input_output_aliases={8: 0, 9: 1},
        name="last_scores",
        compiler_params=pltpu.CompilerParams(vmem_limit_bytes=10 << 20),
    )(ids, *vmem(centroids), cent_norm, *rows, ahead, codes, state[2], *state[:2])


def side_scores(ids, centroids, cent_norm, sides, pieces, state, at, n_slots, half, sharpness):
    feat = centroids.shape[1]
    n_rows = n_slots * BLOCK
    fresh = isinstance(state[0], jax.ShapeDtypeStruct)
    n_in = len(sides[0])

    def body(ids_ref, cents_ref, norm_ref, *refs):
        x_refs, y_refs = refs[:n_in], refs[n_in : 2 * n_in]
        x_rows, y_rows, x_out, y_out = refs[len(refs) - 4 :]
        step = pl.program_id(0)

        def score(rows_ref):
            return sharpness * (2.0 * product(cents_ref, rows_ref) - norm_ref[...])

        @pl.when(step == 0)
        def _():
            keep(x_refs, pieces, x_rows)
            keep(y_refs, pieces, y_rows)

        @pl.when(step != 3)
        def _():
            x_out[...] = score(x_rows)

        @pl.when(step != 2)
        def _():
            y_out[...] = score(y_rows)

    def block(i, ids):
        mine = ids[1]
        other = jnp.where(i == 2, 2 * (mine ^ 2) + 1, 2 * (mine ^ 1))
        return (jnp.where(i < 2, 2 * mine + i, other), 0)

    grid_spec = pltpu.PrefetchScalarGridSpec(
        num_scalar_prefetch=1,
        grid=(4,),
        in_specs=[pl.BlockSpec((half, feat), block), pl.BlockSpec((half, 1), block)]
        + [pl.BlockSpec(r.shape, lambda i, ids: (0, 0)) for r in sides[0] + sides[1]]
        + ([] if fresh else [ANY] * 4),
        out_specs=[
            pl.BlockSpec((n_rows, feat), lambda i, ids: (at, 0)),
            pl.BlockSpec((n_rows, feat), lambda i, ids: (at, 0)),
            pl.BlockSpec((half, n_rows), lambda i, ids: (jnp.minimum(i, 2), at)),
            pl.BlockSpec((half, n_rows), lambda i, ids: (jnp.where(i == 3, 2, jnp.minimum(i, 1)), at)),
        ],
    )
    return pl.pallas_call(
        body,
        out_shape=[pltpu.VMEM(v.shape, v.dtype) for v in state],
        grid_spec=grid_spec,
        input_output_aliases={} if fresh else {3 + 2 * n_in + i: i for i in range(4)},
        name="side_scores",
        compiler_params=pltpu.CompilerParams(vmem_limit_bytes=12 << 20),
    )(ids, *vmem(centroids), cent_norm, *sides[0], *sides[1], *([] if fresh else state))


def one_side_scores(ids, centroids, cent_norm, rows, pieces, state, at, n_slots, half, sharpness, bit):
    feat = centroids.shape[1]
    n_rows = n_slots * BLOCK
    n_in = len(rows)

    def body(ids_ref, cents_ref, norm_ref, *refs):
        rows_out, score_out = refs[len(refs) - 2 :]

        keep(refs[:n_in], pieces, rows_out)
        mine = ids_ref[1]
        other = 2 * (mine ^ 2) + 1 if bit == 1 else 2 * (mine ^ 1)
        for first, block, count in ((0, 2 * mine, 2 * half), (2 * half, other, half)):
            span = pl.ds(pl.multiple_of(block * half, half), count)
            score = sharpness * (2.0 * product(cents_ref.at[span], rows_out) - norm_ref[span, :])
            score_out[first : first + count, :] = score

    grid_spec = pltpu.PrefetchScalarGridSpec(
        num_scalar_prefetch=1,
        grid=(1,),
        in_specs=[
            pl.BlockSpec(centroids.shape, lambda i, ids: (0, 0)),
            pl.BlockSpec(cent_norm.shape, lambda i, ids: (0, 0)),
        ]
        + [pl.BlockSpec(r.shape, lambda i, ids: (0, 0)) for r in rows]
        + [ANY] * 2,
        out_specs=[
            pl.BlockSpec((n_rows, feat), lambda i, ids: (at, 0)),
            pl.BlockSpec((3 * half, n_rows), lambda i, ids: (0, at)),
        ],
    )
    return pl.pallas_call(
        body,
        out_shape=[pltpu.VMEM(v.shape, v.dtype) for v in state],
        grid_spec=grid_spec,
        input_output_aliases={3 + n_in + i: i for i in range(2)},
        name="one_side_scores",
        compiler_params=pltpu.CompilerParams(vmem_limit_bytes=20 << 20),
    )(ids, *vmem(centroids), cent_norm, *rows, *state)


def log_total(kept):
    peak = jnp.maximum(jnp.max(kept, axis=0, keepdims=True), 0.0)
    mass = jnp.sum(jnp.exp(kept - peak), axis=0, keepdims=True)
    return peak + jnp.log(jnp.exp(-peak) + mass)


def combine(notes, seq, block_count):
    n_mp = 2 * len(notes)

    def body(*refs):
        note_refs, (slot_ref, row_ref) = refs[: len(notes)], refs[len(notes) :]

        def rows(j, first, count):
            start = 2 * n_mp * (j % 2) + first
            return note_refs[j // 2][start : start + count, :]

        for i, k in enumerate(seq):
            lse = jnp.concatenate([rows(k ^ j, at, 1) for at, j in enumerate(seq)], axis=0)
            code = rows(k, n_mp, n_mp)
            mine = code[i : i + 1, :]
            total = log_total(jnp.where((code == mine) & (code > 0.0), lse, -NEVER))
            slot_ref[i : i + 1, :] = jnp.where(mine > 0.0, total, NEVER)
            if k == 0:
                for b in range(block_count):
                    row_ref[b : b + 1, :] = log_total(jnp.where(code == float(b + 1), lse, -NEVER))

    return call(
        body,
        [jax.ShapeDtypeStruct((n_mp, LANES), F32), jax.ShapeDtypeStruct((block_count, LANES), F32)],
        [VMEM] * len(notes),
        [VMEM, VMEM],
    )(*notes)


def weights_of(score_ref, norm_ref, into, column, total):
    for k in range(norm_ref.shape[0]):
        tile = jnp.exp(score_ref[:, k * BLOCK : (k + 1) * BLOCK] - norm_ref[k : k + 1, :])
        total = tile if total is None else total + tile
        into[:, column + k * BLOCK : column + (k + 1) * BLOCK] = tile.astype(BF16)
    return total


def sent_sums(side_rows, side_score, norms, half, first, columns, tile, with_counts):
    n_rows = side_rows[0].shape[0]
    steps = columns // tile

    def body(x_ref, y_ref, xs_ref, ys_ref, xn_ref, yn_ref, x_out, y_out, w_buf, c_buf):
        step = pl.program_id(0)

        @pl.when(step == 0)
        def _():
            for i, (s_ref, n_ref) in enumerate(((xs_ref, xn_ref), (ys_ref, yn_ref))):
                total = weights_of(s_ref, n_ref, w_buf.at[i], 0, None)
                c_buf[i] = jnp.broadcast_to(jnp.sum(total, axis=1, keepdims=True), c_buf.shape[1:])

        for i, (r_ref, out) in enumerate(((x_ref, x_out), (y_ref, y_out))):
            counts = c_buf[i]

            @pl.when(step < steps)
            def _():
                part = jnp.dot(w_buf[i], r_ref[...], preferred_element_type=F32)
                out[...] = part * (2.0**10 / jnp.maximum(counts[:, 0:1], 2.0**-20))

            @pl.when(step == steps)
            def _():
                hi = counts.astype(BF16).astype(F32)
                mid = (counts - hi).astype(BF16).astype(F32)
                low = (counts - hi - mid).astype(BF16).astype(F32)
                lane = lax.broadcasted_iota(jnp.int32, counts.shape, 1)
                terms = jnp.where(lane == 0, hi, jnp.where(lane == 1, mid, jnp.where(lane == 2, low, 0.0)))
                out[:, :LANES] = terms

    base = first // tile
    rows_spec = pl.BlockSpec((n_rows, tile), lambda i: (0, base + jnp.minimum(i, steps - 1)))
    score_spec = pl.BlockSpec((half, n_rows), lambda i: (2, 0))
    norm_spec = pl.BlockSpec(norms[0].shape, lambda i: (0, 0))
    out_spec = pl.BlockSpec((half, tile), lambda i: (0, i))
    width = columns + LANES if with_counts else columns
    return pl.pallas_call(
        body,
        out_shape=[jax.ShapeDtypeStruct((half, width), F32)] * 2,
        grid=(steps + 1 if with_counts else steps,),
        in_specs=[rows_spec] * 2 + [score_spec] * 2 + [norm_spec] * 2,
        out_specs=[out_spec] * 2,
        scratch_shapes=[pltpu.VMEM((2, half, n_rows), BF16), pltpu.VMEM((2, half, LANES), F32)],
        name="sent_sums",
        compiler_params=pltpu.CompilerParams(vmem_limit_bytes=16 << 20),
    )(*vmem(*side_rows, *side_score), *norms)


def own_sums(rows, scores, norms, width, tile):
    n_rows, feat = rows[0].shape

    def body(a_ref, b_ref, c_ref, as_ref, bs_ref, cs_ref, an_ref, bn_ref, cn_ref, out_ref, count_ref, w_buf):
        @pl.when(pl.program_id(0) == 0)
        def _():
            total = None
            for i, (s_ref, n_ref) in enumerate(((as_ref, an_ref), (bs_ref, bn_ref), (cs_ref, cn_ref))):
                total = weights_of(s_ref, n_ref, w_buf, i * n_rows, total)
            count_ref[...] = jnp.sum(total, axis=1, keepdims=True)

        acc = jnp.dot(w_buf[:, :n_rows], a_ref[...], preferred_element_type=F32)
        acc += jnp.dot(w_buf[:, n_rows : 2 * n_rows], b_ref[...], preferred_element_type=F32)
        acc += jnp.dot(w_buf[:, 2 * n_rows :], c_ref[...], preferred_element_type=F32)
        out_ref[...] = acc

    return pl.pallas_call(
        body,
        out_shape=[pltpu.VMEM((width, feat), F32), jax.ShapeDtypeStruct((width, 1), F32)],
        grid=(feat // tile,),
        in_specs=[pl.BlockSpec((n_rows, tile), lambda i: (0, i))] * 3
        + [pl.BlockSpec((width, n_rows), lambda i: (0, 0))] * 3
        + [pl.BlockSpec(norms[0].shape, lambda i: (0, 0))] * 3,
        out_specs=[
            pl.BlockSpec((width, tile), lambda i: (0, i)),
            pl.BlockSpec((width, 1), lambda i: (0, 0)),
        ],
        scratch_shapes=[pltpu.VMEM((width, 3 * n_rows), BF16)],
        name="own_sums",
        compiler_params=pltpu.CompilerParams(vmem_limit_bytes=24 << 20),
    )(*vmem(*rows, *scores), *norms)


def update(ids, own, counts, parts, centroids, first, columns, state, final, n_devices):
    width, feat = own.shape
    half = width // 2
    at = first // columns

    def body(ids_ref, own_ref, count_ref, a_ref, b_ref, old_ref, *refs):
        tails = refs[:2]
        new_ref, *refs = refs[3:] + refs[:2] if final else refs[2:]
        tops = []
        for i, part_ref in enumerate((a_ref, b_ref)):
            span = slice(i * half, (i + 1) * half)
            if final:
                sent, before_square = refs[2][span, :], refs[3][span, :]
            else:
                tail = tails[i]
                lane = lax.broadcasted_iota(jnp.int32, (half, LANES), 1)
                sent = jnp.sum(jnp.where(lane < 3, tail[...], 0.0), axis=1, keepdims=True)
                before_square = 0.0
                refs[1][span, :] = sent
            back = part_ref[...] * (jnp.maximum(sent, 2.0**-20) * 2.0**-10)
            before = old_ref[span, :].astype(F32)
            after = (own_ref[span, :] + back + before) / (count_ref[span, :] + sent + 1.0)
            new_ref[span, :] = after
            total = before_square + jnp.sum(jnp.square(after - before), axis=1, keepdims=True)
            if final:
                total = jnp.sqrt(total + 1.0)
                tops.append(jnp.max(total, axis=0, keepdims=True))
            refs[0][span, :] = total
        if final:
            refs[1][...] = jnp.broadcast_to(jnp.maximum(*tops), refs[1].shape)

    def whole(shape):
        return pl.BlockSpec(shape, lambda i, ids: (0, 0))

    block = pl.BlockSpec((width, columns), lambda i, ids: (0, at))
    thin = jax.ShapeDtypeStruct((width, 1), F32)
    out_shape = [jax.ShapeDtypeStruct((width, feat), F32), thin]
    out_specs = [block, whole((width, 1))]
    if final:
        new, square, sent = state
        extra, extra_specs = [sent, square, new], [whole((width, 1))] * 2 + [ANY]
        out_shape.append(jax.ShapeDtypeStruct((n_devices, LANES), F32))
        out_specs.append(whole((n_devices, LANES)))
    else:
        extra, extra_specs = parts, [pl.BlockSpec((half, LANES), lambda i, ids: (0, columns // LANES))] * 2
        out_shape.append(thin)
        out_specs.append(whole((width, 1)))
    return pl.pallas_call(
        body,
        out_shape=out_shape,
        grid_spec=pltpu.PrefetchScalarGridSpec(
            num_scalar_prefetch=1,
            grid=(1,),
            in_specs=[block, whole((width, 1))]
            + [whole((half, columns))] * 2
            + [pl.BlockSpec((width, columns), lambda i, ids: (ids[1], at))]
            + extra_specs,
            out_specs=out_specs,
        ),
        input_output_aliases={8: 0} if final else {},
        name="update",
        compiler_params=pltpu.CompilerParams(vmem_limit_bytes=16 << 20),
    )(ids, *vmem(own), counts, *parts, *vmem(centroids), *extra)


def sequence(n_mp):
    return [0, 1, 6, 2, 3, 7, 4, 5] if n_mp == 8 else list(range(n_mp))


def pieces_of(n_mp, feat):
    mid = feat // 2
    seq = sequence(n_mp)
    return [[(k, 0, feat)] if at < n_mp - 3 else [(k, 0, mid), (k, mid, mid)] for at, k in enumerate(seq)]


def own_groups(n_mp):
    return [(k, k + 1) for k in range(0, n_mp - 2, 2)] + [(n_mp - 2,)]


def on_square(data_rows, centroids, block_mask, lower_bound):
    feat = data_rows.shape[1]
    width = centroids.shape[0]
    block_count = data_rows.shape[0] // BLOCK
    n_mp = lax.axis_size("mp")
    n_dp = lax.axis_size("dp")
    own_width = width // n_dp
    half = own_width // 2
    my_mp = lax.axis_index("mp").astype(jnp.int32)
    my_dp = lax.axis_index("dp").astype(jnp.int32)
    sharpness = 4.0 / math.sqrt(feat)
    ids = jnp.stack([my_mp, my_dp])
    mask_t = block_mask.T

    seq = sequence(n_mp)
    last = seq[-1]
    cuts = {cut[0][0]: cut for cut in pieces_of(n_mp, feat)}
    early = [p for k in seq[2:5] for p in cuts[k]]
    late = cuts[0] + [p for k in seq[5:] for p in cuts[k]] + cuts[1]
    got = dict(zip(early, take_slots(ids, mask_t, data_rows, early, [])))
    *rest, codes = take_slots(ids, mask_t, data_rows, late, seq)
    got.update(zip(late, rest))
    for piece in early + late[1:]:
        got[piece] = swap(got[piece], "mp", n_mp, piece[0])

    side = {}
    for k in seq:
        for piece in cuts[k]:
            for bit in (1, 2):
                side[bit, piece] = swap(got[piece], "dp", n_dp, bit)

    cents, cent_norm = load_centroids(centroids, 2 * n_dp)

    n_rows = n_mp * BLOCK
    own = [
        jax.ShapeDtypeStruct((n_rows, feat), BF16),
        jax.ShapeDtypeStruct((own_width, n_rows), F32),
        jax.ShapeDtypeStruct((n_mp, 1, BLOCK), F32),
    ]
    sides = [jax.ShapeDtypeStruct((n_rows, feat), BF16)] * 2
    sides += [jax.ShapeDtypeStruct((3 * half, n_rows), F32)] * 2
    ahead = first_product(cents, got[cuts[last][0]], n_dp)
    for group in own_groups(n_mp):
        held = [p for at in group for p in cuts[seq[at]]]
        placed = [(seq.index(p[0]) - group[0], p[1], p[2]) for p in held]
        own = own_scores(
            ids, cents, cent_norm, [got[p] for p in held], placed, own, group[0] // len(group), len(group),
            n_dp, sharpness,
        )
    for i in range(n_mp // 2):
        held = cuts[seq[2 * i]] + cuts[seq[2 * i + 1]]
        placed = [(seq.index(p[0]) - 2 * i, p[1], p[2]) for p in held]
        pair = [[side[bit, p] for p in held] for bit in (1, 2)]
        if i < n_mp // 2 - 1:
            sides = list(side_scores(ids, cents, cent_norm, pair, placed, sides, i, 2, half, sharpness))
            continue
        for bit in (1, 2):
            sides[bit - 1 :: 2] = one_side_scores(
                ids, cents, cent_norm, pair[bit - 1], placed, sides[bit - 1 :: 2], i, 2, half, sharpness, bit
            )

    *own, note = last_scores(ids, cents, cent_norm, [got[p] for p in cuts[last]], ahead, codes, own, n_dp, sharpness)
    beside = swap(note, "mp", n_mp, 1)
    both = jnp.concatenate([note, beside])
    notes = [both]
    for k in range(2, n_mp, 2):
        notes.append(swap(both, "mp", n_mp, k))
    slot_norm, row_norm = combine(notes, seq, block_count)
    log_norm = row_norm.reshape(-1)
    side_norm = []
    for bit in (1, 2):
        side_norm.append(swap(slot_norm, "dp", n_dp, bit))

    tile = feat // 4
    spans = [(0, 2 * tile), (2 * tile, 2 * tile)]
    received = []
    for i, (first, columns) in enumerate(spans):
        sent = sent_sums(sides[:2], sides[2:], side_norm, half, first, columns, tile, i == 0)
        for_y, for_x = [v.astype(jnp.float16) for v in sent]
        pair = []
        for bit, message in ((1, for_x), (2, for_y)):
            pair.append(swap(message, "dp", n_dp, bit).astype(F32))
        received.append(pair)
    total, counts = own_sums(
        [own[0], sides[0], sides[1]], [own[1], sides[2], sides[3]], [slot_norm] + side_norm, own_width, tile
    )
    state = None
    for i, (first, columns) in enumerate(spans):
        state = update(ids, total, counts, received[i], cents, first, columns, state, i == len(spans) - 1, n_dp * n_mp)
    updated, movement, peak = state
    shard_peaks = lax.all_to_all(peak, ("dp", "mp"), split_axis=0, concat_axis=0, tiled=True)
    shard_peak = jnp.max(shard_peaks.reshape(n_dp, n_mp, LANES), axis=(0, 2))
    new_lower = lower_bound - shard_peak[:, None]
    return (updated, movement[:, 0], log_norm, new_lower)


def on_device(data_rows, centroids, block_mask, lower_bound):
    feat = data_rows.shape[1]
    width = centroids.shape[0]
    block_count = data_rows.shape[0] // BLOCK
    n_mp = lax.axis_size("mp")
    n_dp = lax.axis_size("dp")
    own_width = width // n_dp
    my_mp = lax.axis_index("mp")
    my_dp = lax.axis_index("dp")
    sharpness = 4.0 / math.sqrt(feat)

    labels = jnp.arange(1, block_count + 1, dtype=jnp.int32)
    codes = jnp.sum(block_mask * labels[None, :], axis=1)

    def outgoing(k):
        code = lax.dynamic_index_in_dim(codes, my_mp ^ k, 0, keepdims=False)
        start = jnp.maximum(code - 1, 0) * BLOCK
        return lax.dynamic_slice(data_rows, (start, 0), (BLOCK, feat))

    order = list(range(2, n_mp)) + [1]
    got = {0: outgoing(0)}
    for k in order:
        got[k] = swap(outgoing(k), "mp", n_mp, k)

    cent_norm = jnp.sum(jnp.square(centroids.astype(jnp.float32)), axis=1)

    scores, lses = {}, {}
    groups = [(k, k + 1) for k in range(0, n_mp, 2)]
    for group in groups:
        rows = jnp.concatenate([got[k] for k in group], axis=0)
        product = lax.dot_general(
            centroids, rows, (((1,), (1,)), ((), ())), preferred_element_type=jnp.float32
        )
        score = sharpness * (2.0 * product - cent_norm[:, None])
        top = jnp.max(score, axis=0)
        lse = top + jnp.log(jnp.sum(jnp.exp(score - top[None, :]), axis=0))
        scores[group] = score
        for i, k in enumerate(group):
            lses[k] = lse[i * BLOCK : (i + 1) * BLOCK]

    note = jnp.concatenate(
        [
            jnp.stack([lses[k] for k in range(n_mp)]),
            jnp.pad(codes.astype(jnp.float32), (0, BLOCK - n_mp))[None, :],
        ]
    )
    notes = lax.all_to_all(
        jnp.broadcast_to(note[None], (n_mp,) + note.shape), "mp", split_axis=0, concat_axis=0, tiled=True
    )
    shard_ids = jnp.arange(n_mp, dtype=jnp.int32)
    lse_of = notes[:, :n_mp, :]
    all_code = notes[:, n_mp, :n_mp].astype(jnp.int32)
    all_lse = lse_of[shard_ids[None, :], shard_ids[None, :] ^ shard_ids[:, None]]
    tops = jnp.where((all_code > 0)[:, :, None], all_lse, -1e30)

    def normalizer(same, lse):
        kept = jnp.where(same[:, :, None], lse, -1e30)
        peak = jnp.maximum(jnp.max(kept, axis=1), 0.0)
        mass = jnp.sum(jnp.exp(kept - peak[:, None, :]), axis=1)
        return peak + jnp.log(jnp.exp(-peak) + mass)

    my_lse = lax.dynamic_index_in_dim(tops, my_mp, 0, keepdims=False)
    row_norm = normalizer(codes[None, :] == labels[:, None], jnp.broadcast_to(my_lse[None], (block_count,) + my_lse.shape))
    log_norm = row_norm.reshape(-1)

    slot_code = lax.dynamic_index_in_dim(all_code, my_mp, 1, keepdims=False)
    slot_norm = normalizer((all_code == slot_code[:, None]) & (all_code > 0), tops)

    weights, counts = [], 0.0
    for group in groups:
        src = [my_mp ^ k for k in group]
        norm = jnp.concatenate([slot_norm[m] for m in src])
        valid = jnp.concatenate([jnp.broadcast_to(slot_code[m] > 0, (BLOCK,)) for m in src])
        weight = jnp.where(valid[None, :], jnp.exp(scores[group] - norm[None, :]), 0.0)
        counts = counts + jnp.sum(weight, axis=1)
        weights.append(weight.astype(jnp.bfloat16))
    weight_half = jnp.concatenate(weights, axis=1)
    rows = jnp.concatenate([got[k] for k in range(n_mp)], axis=0)

    def quarter(j):
        return (my_dp ^ j) * own_width

    def partial(j, half):
        w = lax.dynamic_slice(weight_half, (quarter(j), 0), (own_width, weight_half.shape[1]))
        x = lax.slice_in_dim(rows, half * (feat // 2), (half + 1) * (feat // 2), axis=1)
        return lax.dot_general(w, x, (((1,), (0,)), ((), ())), preferred_element_type=jnp.float32)

    count_of = {0: counts}
    for j in range(1, n_dp):
        count_of[j] = swap(counts, "dp", n_dp, j)

    def sub(vec, j):
        return lax.dynamic_slice(vec, (quarter(j),), (own_width,))

    def scale(members, j):
        total = sum(sub(count_of[i], j) for i in members)
        return jnp.maximum(total, 2.0**-20)[:, None] * 2.0**-10

    bits = [1 << b for b in range(n_dp.bit_length() - 1)]
    plan = [bits, bits[::-1]]
    current = [{}, {}]
    for j in reversed(range(n_dp)):
        for half in range(2):
            jj = j if half == 0 or n_dp != 4 else {3: 3, 1: 2, 2: 1, 0: 0}[j]
            current[half][jj] = None
    todo = [[j for j in reversed(range(n_dp))] for _ in range(2)]
    for half in range(2):
        for j in todo[half]:
            current[half][j] = partial(j, half)
    members = [{0}, {0}]
    for step in range(len(bits)):
        for half in range(2):
            bit = plan[half][step]
            cur = current[half]
            mine = members[half]
            theirs = {i ^ bit for i in mine}
            kept = {}
            for j in sorted(cur, reverse=True):
                if not j & bit:
                    continue
                sent = (cur[j] / scale(mine, j)).astype(jnp.float16)
                back = swap(sent, "dp", n_dp, bit)
                kept[j ^ bit] = cur[j ^ bit] + back.astype(jnp.float32) * scale(theirs, j ^ bit)
            current[half] = kept
            members[half] = mine | theirs
    part_sums = jnp.concatenate([current[0][0], current[1][0]], axis=1)
    part_counts = sum(sub(count_of[j], 0) for j in range(n_dp))

    old_cents = lax.dynamic_slice_in_dim(centroids, my_dp * own_width, own_width, 0).astype(jnp.float32)
    updated = (part_sums + old_cents) / (part_counts[:, None] + 1.0)
    movement = jnp.sqrt(jnp.sum(jnp.square(updated - old_cents), axis=1) + 1.0)
    peak = jnp.broadcast_to(jnp.max(movement), (n_dp * n_mp, 1))
    shard_peaks = lax.all_to_all(peak, ("dp", "mp"), split_axis=0, concat_axis=0, tiled=True)
    shard_peak = jnp.max(shard_peaks.reshape(n_dp, n_mp), axis=0)
    new_lower = lower_bound - shard_peak[:, None]
    return (updated, movement, log_norm, new_lower)


def solution(mesh):
    placed = (P(("dp", "mp"), None), P("mp", None), P(None, ("dp", "mp")), P(None, ("dp", "mp")))
    square = mesh.shape["dp"] == 4

    def body(*args):
        return on_square(*args) if square else on_device(*args)

    return jax.shard_map(
        body,
        mesh=mesh,
        in_specs=placed,
        out_specs=(P(("mp", "dp"), None), P(("mp", "dp")), P(("dp", "mp")), P(None, ("dp", "mp"))),
        check_vma=False,
    )
```

```python
import math

import jax
import jax.numpy as jnp
from jax import lax
from jax.experimental import pallas as pl
from jax.experimental.pallas import tpu as pltpu
from jax.sharding import PartitionSpec as P


BLOCK = 128
LANES = 128
F32 = jnp.float32
BF16 = jnp.bfloat16
NEVER = 1e30
ANY = pl.BlockSpec(memory_space=pl.ANY)
SMEM = pl.BlockSpec(memory_space=pltpu.SMEM)
VMEM = pl.BlockSpec(memory_space=pltpu.VMEM)


def hbm(*arrays):
    return [pltpu.with_memory_space_constraint(v, pltpu.HBM) for v in arrays]


def vmem(*arrays):
    return [pltpu.with_memory_space_constraint(v, pltpu.VMEM) for v in arrays]


def swap(value, axis, size, offset):
    return lax.ppermute(value, axis, [(i, i ^ offset) for i in range(size)])


def call(body, out_shape, in_specs, out_specs, scratch=(), vmem=4):
    return pl.pallas_call(
        body,
        out_shape=out_shape,
        in_specs=in_specs,
        out_specs=out_specs,
        scratch_shapes=list(scratch),
        compiler_params=pltpu.CompilerParams(vmem_limit_bytes=vmem << 20),
    )


def take_slots(ids, mask_t, data_rows, pieces, coded):
    block_count, n_mp = mask_t.shape

    def body(ids_ref, mask_ref, rows_ref, *refs):
        outs, sems = refs[:-1], refs[-1]

        def code_of(k):
            shard = ids_ref[0] ^ k
            code = mask_ref[0, shard]
            for b in range(1, block_count):
                code = code + (b + 1) * mask_ref[b, shard]
            return code

        copies = []
        for i, (k, first, count) in enumerate(pieces):
            start = jnp.maximum(code_of(k) - 1, 0) * BLOCK
            src = rows_ref.at[pl.ds(pl.multiple_of(start, BLOCK), BLOCK), pl.ds(first, count)]
            copies.append(pltpu.make_async_copy(src, outs[i], sems.at[i]))
            copies[-1].start()
        for i, k in enumerate(coded):
            outs[-1][i : i + 1, :] = jnp.full((1, LANES), code_of(k), jnp.int32).astype(F32)
        for copy in copies:
            copy.wait()

    shapes = [pltpu.VMEM((BLOCK, count), data_rows.dtype) for _, _, count in pieces]
    if coded:
        shapes.append(jax.ShapeDtypeStruct((n_mp, LANES), F32))
    return call(
        body, shapes, [SMEM, SMEM, ANY], [VMEM] * len(shapes), [pltpu.SemaphoreType.DMA((len(pieces),))], 8
    )(ids, mask_t, *hbm(data_rows))


def load_centroids(centroids, n_parts):
    width, feat = centroids.shape
    part = width // n_parts

    def body(in_ref, out_ref, norm_ref):
        values = in_ref[...]
        out_ref[...] = values
        norm_ref[...] = jnp.sum(jnp.square(values.astype(F32)), axis=1, keepdims=True)

    return pl.pallas_call(
        body,
        out_shape=[pltpu.VMEM((width, feat), centroids.dtype), jax.ShapeDtypeStruct((width, 1), F32)],
        grid=(n_parts,),
        in_specs=[pl.BlockSpec((part, feat), lambda i: (i, 0))],
        out_specs=[pl.BlockSpec((part, feat), lambda i: (i, 0)), pl.BlockSpec((part, 1), lambda i: (i, 0))],
        name="load_centroids",
        compiler_params=pltpu.CompilerParams(vmem_limit_bytes=10 << 20),
    )(*hbm(centroids))


def product(cents_ref, rows_ref):
    return lax.dot_general(
        cents_ref[...], rows_ref[...], (((1,), (1,)), ((), ())), preferred_element_type=F32
    )


def keep(row_refs, pieces, out_ref):
    for ref, (place, first, count) in zip(row_refs, pieces):
        out_ref[place * BLOCK : (place + 1) * BLOCK, first : first + count] = ref[...]


def own_scores(ids, centroids, cent_norm, rows, pieces, state, at, n_slots, n_parts, sharpness):
    width, feat = centroids.shape
    part = width // n_parts
    n_rows = n_slots * BLOCK
    fresh = isinstance(state[0], jax.ShapeDtypeStruct)
    n_in = len(rows)

    def body(ids_ref, cents_ref, norm_ref, *refs):
        row_refs = refs[:n_in]
        rows_out, score_out, lse_out, score_buf = refs[len(refs) - 4 :]

        keep(row_refs, pieces, rows_out)
        score_buf[...] = sharpness * (2.0 * product(cents_ref, rows_out) - norm_ref[...])
        score_out[...] = score_buf[pl.ds(pl.multiple_of(ids_ref[1] * part, part), part), :]
        top = jnp.max(score_buf[...], axis=0, keepdims=True)
        lse = top + jnp.log(jnp.sum(jnp.exp(score_buf[...] - top), axis=0, keepdims=True))
        for i in range(n_slots):
            lse_out[i] = lse[:, i * BLOCK : (i + 1) * BLOCK]

    grid_spec = pltpu.PrefetchScalarGridSpec(
        num_scalar_prefetch=1,
        grid=(1,),
        in_specs=[
            pl.BlockSpec((width, feat), lambda i, ids: (0, 0)),
            pl.BlockSpec((width, 1), lambda i, ids: (0, 0)),
        ]
        + [pl.BlockSpec(r.shape, lambda i, ids: (0, 0)) for r in rows]
        + ([] if fresh else [ANY] * 3),
        out_specs=[
            pl.BlockSpec((n_rows, feat), lambda i, ids: (at, 0)),
            pl.BlockSpec((part, n_rows), lambda i, ids: (0, at)),
            pl.BlockSpec((n_slots, 1, BLOCK), lambda i, ids: (at, 0, 0)),
        ],
        scratch_shapes=[pltpu.VMEM((width, n_rows), F32)],
    )
    return pl.pallas_call(
        body,
        out_shape=[pltpu.VMEM(v.shape, v.dtype) for v in state],
        grid_spec=grid_spec,
        input_output_aliases={} if fresh else {3 + n_in + i: i for i in range(3)},
        name="own_scores",
        compiler_params=pltpu.CompilerParams(vmem_limit_bytes=20 << 20),
    )(ids, *vmem(centroids), cent_norm, *rows, *([] if fresh else state))


def first_product(centroids, rows, n_parts):
    width = centroids.shape[0]
    columns = rows.shape[1]
    part = width // n_parts

    def body(cents_ref, rows_ref, out_ref):
        out_ref[...] = product(cents_ref, rows_ref)

    return pl.pallas_call(
        body,
        out_shape=pltpu.VMEM((width, BLOCK), F32),
        grid=(n_parts,),
        in_specs=[
            pl.BlockSpec((part, columns), lambda i: (i, 0)),
            pl.BlockSpec((BLOCK, columns), lambda i: (0, 0)),
        ],
        out_specs=pl.BlockSpec((part, BLOCK), lambda i: (i, 0)),
        name="first_product",
        compiler_params=pltpu.CompilerParams(vmem_limit_bytes=8 << 20),
    )(*vmem(centroids), rows)


def last_scores(ids, centroids, cent_norm, rows, ahead, codes, state, n_parts, sharpness):
    width, feat = centroids.shape
    part = width // n_parts
    mid = feat // 2
    n_mp = codes.shape[0]
    last = n_mp - 1

    def body(ids_ref, cents_ref, norm_ref, a_ref, b_ref, ahead_ref, code_ref, lse_ref, *refs):
        rows_out, score_out, note_ref, score_buf = refs[len(refs) - 4 :]
        rows_out[:, :mid] = a_ref[...]
        rows_out[:, mid:] = b_ref[...]
        for k in range(last):
            note_ref[k : k + 1, :] = lse_ref[k]
        note_ref[n_mp:, :] = code_ref[...]
        score_buf[...] = sharpness * (2.0 * (ahead_ref[...] + product(cents_ref, b_ref)) - norm_ref[...])
        score_out[...] = score_buf[pl.ds(pl.multiple_of(ids_ref[1] * part, part), part), :]
        top = jnp.max(score_buf[...], axis=0, keepdims=True)
        mass = jnp.sum(jnp.exp(score_buf[...] - top), axis=0, keepdims=True)
        note_ref[last : last + 1, :] = top + jnp.log(mass)

    def whole(shape):
        return pl.BlockSpec(shape, lambda i, ids: (0,) * len(shape))

    grid_spec = pltpu.PrefetchScalarGridSpec(
        num_scalar_prefetch=1,
        grid=(1,),
        in_specs=[
            pl.BlockSpec((width, mid), lambda i, ids: (0, 1)),
            pl.BlockSpec((width, 1), lambda i, ids: (0, 0)),
            whole((BLOCK, mid)),
            whole((BLOCK, mid)),
            pl.BlockSpec((width, BLOCK), lambda i, ids: (0, 0)),
            whole(codes.shape),
            whole(state[2].shape),
            ANY,
            ANY,
        ],
        out_specs=[
            pl.BlockSpec((BLOCK, feat), lambda i, ids: (last, 0)),
            pl.BlockSpec((part, BLOCK), lambda i, ids: (0, last)),
            whole((2 * n_mp, LANES)),
        ],
        scratch_shapes=[pltpu.VMEM((width, BLOCK), F32)],
    )
    return pl.pallas_call(
        body,
        out_shape=[pltpu.VMEM(v.shape, v.dtype) for v in state[:2]]
        + [jax.ShapeDtypeStruct((2 * n_mp, LANES), F32)],
        grid_spec=grid_spec,
        input_output_aliases={8: 0, 9: 1},
        name="last_scores",
        compiler_params=pltpu.CompilerParams(vmem_limit_bytes=16 << 20),
    )(ids, *vmem(centroids), cent_norm, *rows, ahead, codes, state[2], *state[:2])


def one_side_scores(ids, centroids, cent_norm, rows, pieces, state, at, n_slots, half, sharpness, bit):
    feat = centroids.shape[1]
    fresh = isinstance(state[0], jax.ShapeDtypeStruct)
    n_rows = n_slots * BLOCK
    n_in = len(rows)

    def body(ids_ref, cents_ref, norm_ref, *refs):
        rows_out, score_out = refs[len(refs) - 2 :]

        keep(refs[:n_in], pieces, rows_out)
        mine = ids_ref[1]
        other = 2 * (mine ^ 2) + 1 if bit == 1 else 2 * (mine ^ 1)
        for first, block, count in ((0, 2 * mine, 2 * half), (2 * half, other, half)):
            span = pl.ds(pl.multiple_of(block * half, half), count)
            score = sharpness * (2.0 * product(cents_ref.at[span], rows_out) - norm_ref[span, :])
            score_out[first : first + count, :] = score

    grid_spec = pltpu.PrefetchScalarGridSpec(
        num_scalar_prefetch=1,
        grid=(1,),
        in_specs=[
            pl.BlockSpec(centroids.shape, lambda i, ids: (0, 0)),
            pl.BlockSpec(cent_norm.shape, lambda i, ids: (0, 0)),
        ]
        + [pl.BlockSpec(r.shape, lambda i, ids: (0, 0)) for r in rows]
        + ([] if fresh else [ANY] * 2),
        out_specs=[
            pl.BlockSpec((n_rows, feat), lambda i, ids: (at, 0)),
            pl.BlockSpec((3 * half, n_rows), lambda i, ids: (0, at)),
        ],
    )
    return pl.pallas_call(
        body,
        out_shape=[pltpu.VMEM(v.shape, v.dtype) for v in state],
        grid_spec=grid_spec,
        input_output_aliases={} if fresh else {3 + n_in + i: i for i in range(2)},
        name="one_side_scores",
        compiler_params=pltpu.CompilerParams(vmem_limit_bytes=20 << 20),
    )(ids, *vmem(centroids), cent_norm, *rows, *([] if fresh else state))


def log_total(kept):
    peak = jnp.maximum(jnp.max(kept, axis=0, keepdims=True), 0.0)
    mass = jnp.sum(jnp.exp(kept - peak), axis=0, keepdims=True)
    return peak + jnp.log(jnp.exp(-peak) + mass)


def combine(notes, seq, block_count):
    n_mp = 2 * len(notes)

    def body(*refs):
        note_refs, (slot_ref, row_ref) = refs[: len(notes)], refs[len(notes) :]

        def rows(j, first, count):
            start = 2 * n_mp * (j % 2) + first
            return note_refs[j // 2][start : start + count, :]

        for i, k in enumerate(seq):
            lse = jnp.concatenate([rows(k ^ j, at, 1) for at, j in enumerate(seq)], axis=0)
            code = rows(k, n_mp, n_mp)
            mine = code[i : i + 1, :]
            total = log_total(jnp.where((code == mine) & (code > 0.0), lse, -NEVER))
            slot_ref[i : i + 1, :] = jnp.where(mine > 0.0, total, NEVER)
            if k == 0:
                for b in range(block_count):
                    row_ref[b : b + 1, :] = log_total(jnp.where(code == float(b + 1), lse, -NEVER))

    return call(
        body,
        [jax.ShapeDtypeStruct((n_mp, LANES), F32), jax.ShapeDtypeStruct((block_count, LANES), F32)],
        [VMEM] * len(notes),
        [VMEM, VMEM],
    )(*notes)


def weights_of(score_ref, norm_ref, into, column, total):
    for k in range(norm_ref.shape[0]):
        tile = jnp.exp(score_ref[:, k * BLOCK : (k + 1) * BLOCK] - norm_ref[k : k + 1, :])
        total = tile if total is None else total + tile
        into[:, column + k * BLOCK : column + (k + 1) * BLOCK] = tile.astype(BF16)
    return total


def sent_sums(side_rows, side_score, norms, half, first, columns, tile, with_counts):
    n_rows = side_rows[0].shape[0]
    steps = columns // tile

    def body(x_ref, y_ref, xs_ref, ys_ref, xn_ref, yn_ref, x_out, y_out, w_buf, c_buf):
        step = pl.program_id(0)

        @pl.when(step == 0)
        def _():
            for i, (s_ref, n_ref) in enumerate(((xs_ref, xn_ref), (ys_ref, yn_ref))):
                total = weights_of(s_ref, n_ref, w_buf.at[i], 0, None)
                c_buf[i] = jnp.broadcast_to(jnp.sum(total, axis=1, keepdims=True), c_buf.shape[1:])

        for i, (r_ref, out) in enumerate(((x_ref, x_out), (y_ref, y_out))):
            counts = c_buf[i]

            @pl.when(step < steps)
            def _():
                part = jnp.dot(w_buf[i], r_ref[...], preferred_element_type=F32)
                out[...] = part * (2.0**10 / jnp.maximum(counts[:, 0:1], 2.0**-20))

            @pl.when(step == steps)
            def _():
                hi = counts.astype(BF16).astype(F32)
                mid = (counts - hi).astype(BF16).astype(F32)
                low = (counts - hi - mid).astype(BF16).astype(F32)
                lane = lax.broadcasted_iota(jnp.int32, counts.shape, 1)
                terms = jnp.where(lane == 0, hi, jnp.where(lane == 1, mid, jnp.where(lane == 2, low, 0.0)))
                out[:, :LANES] = terms

    base = first // tile
    rows_spec = pl.BlockSpec((n_rows, tile), lambda i: (0, base + jnp.minimum(i, steps - 1)))
    score_spec = pl.BlockSpec((half, n_rows), lambda i: (2, 0))
    norm_spec = pl.BlockSpec(norms[0].shape, lambda i: (0, 0))
    out_spec = pl.BlockSpec((half, tile), lambda i: (0, i))
    width = columns + LANES if with_counts else columns
    return pl.pallas_call(
        body,
        out_shape=[jax.ShapeDtypeStruct((half, width), F32)] * 2,
        grid=(steps + 1 if with_counts else steps,),
        in_specs=[rows_spec] * 2 + [score_spec] * 2 + [norm_spec] * 2,
        out_specs=[out_spec] * 2,
        scratch_shapes=[pltpu.VMEM((2, half, n_rows), BF16), pltpu.VMEM((2, half, LANES), F32)],
        name="sent_sums",
        compiler_params=pltpu.CompilerParams(vmem_limit_bytes=16 << 20),
    )(*vmem(*side_rows, *side_score), *norms)


def own_sums(rows, scores, norms, width, tile):
    n_rows, feat = rows[0].shape

    def body(a_ref, b_ref, c_ref, as_ref, bs_ref, cs_ref, an_ref, bn_ref, cn_ref, out_ref, count_ref, w_buf):
        @pl.when(pl.program_id(0) == 0)
        def _():
            total = None
            for i, (s_ref, n_ref) in enumerate(((as_ref, an_ref), (bs_ref, bn_ref), (cs_ref, cn_ref))):
                total = weights_of(s_ref, n_ref, w_buf, i * n_rows, total)
            count_ref[...] = jnp.sum(total, axis=1, keepdims=True)

        acc = jnp.dot(w_buf[:, :n_rows], a_ref[...], preferred_element_type=F32)
        acc += jnp.dot(w_buf[:, n_rows : 2 * n_rows], b_ref[...], preferred_element_type=F32)
        acc += jnp.dot(w_buf[:, 2 * n_rows :], c_ref[...], preferred_element_type=F32)
        out_ref[...] = acc

    return pl.pallas_call(
        body,
        out_shape=[pltpu.VMEM((width, feat), F32), jax.ShapeDtypeStruct((width, 1), F32)],
        grid=(feat // tile,),
        in_specs=[pl.BlockSpec((n_rows, tile), lambda i: (0, i))] * 3
        + [pl.BlockSpec((width, n_rows), lambda i: (0, 0))] * 3
        + [pl.BlockSpec(norms[0].shape, lambda i: (0, 0))] * 3,
        out_specs=[
            pl.BlockSpec((width, tile), lambda i: (0, i)),
            pl.BlockSpec((width, 1), lambda i: (0, 0)),
        ],
        scratch_shapes=[pltpu.VMEM((width, 3 * n_rows), BF16)],
        name="own_sums",
        compiler_params=pltpu.CompilerParams(vmem_limit_bytes=24 << 20),
    )(*vmem(*rows, *scores), *norms)


def update(ids, own, counts, parts, centroids, first, columns, state, final, n_devices):
    width, feat = own.shape
    half = width // 2
    at = first // columns

    def body(ids_ref, own_ref, count_ref, a_ref, b_ref, old_ref, *refs):
        tails = refs[:2]
        new_ref, *refs = refs[3:] + refs[:2] if final else refs[2:]
        tops = []
        for i, part_ref in enumerate((a_ref, b_ref)):
            span = slice(i * half, (i + 1) * half)
            if final:
                sent, before_square = refs[2][span, :], refs[3][span, :]
            else:
                tail = tails[i]
                lane = lax.broadcasted_iota(jnp.int32, (half, LANES), 1)
                sent = jnp.sum(jnp.where(lane < 3, tail[...], 0.0), axis=1, keepdims=True)
                before_square = 0.0
                refs[1][span, :] = sent
            back = part_ref[...] * (jnp.maximum(sent, 2.0**-20) * 2.0**-10)
            before = old_ref[span, :].astype(F32)
            after = (own_ref[span, :] + back + before) / (count_ref[span, :] + sent + 1.0)
            new_ref[span, :] = after
            total = before_square + jnp.sum(jnp.square(after - before), axis=1, keepdims=True)
            if final:
                total = jnp.sqrt(total + 1.0)
                tops.append(jnp.max(total, axis=0, keepdims=True))
            refs[0][span, :] = total
        if final:
            refs[1][...] = jnp.broadcast_to(jnp.maximum(*tops), refs[1].shape)

    def whole(shape):
        return pl.BlockSpec(shape, lambda i, ids: (0, 0))

    block = pl.BlockSpec((width, columns), lambda i, ids: (0, at))
    thin = jax.ShapeDtypeStruct((width, 1), F32)
    out_shape = [jax.ShapeDtypeStruct((width, feat), F32), thin]
    out_specs = [block, whole((width, 1))]
    if final:
        new, square, sent = state
        extra, extra_specs = [sent, square, new], [whole((width, 1))] * 2 + [ANY]
        out_shape.append(jax.ShapeDtypeStruct((n_devices, LANES), F32))
        out_specs.append(whole((n_devices, LANES)))
    else:
        extra, extra_specs = parts, [pl.BlockSpec((half, LANES), lambda i, ids: (0, columns // LANES))] * 2
        out_shape.append(thin)
        out_specs.append(whole((width, 1)))
    return pl.pallas_call(
        body,
        out_shape=out_shape,
        grid_spec=pltpu.PrefetchScalarGridSpec(
            num_scalar_prefetch=1,
            grid=(1,),
            in_specs=[block, whole((width, 1))]
            + [whole((half, columns))] * 2
            + [pl.BlockSpec((width, columns), lambda i, ids: (ids[1], at))]
            + extra_specs,
            out_specs=out_specs,
        ),
        input_output_aliases={8: 0} if final else {},
        name="update",
        compiler_params=pltpu.CompilerParams(vmem_limit_bytes=16 << 20),
    )(ids, *vmem(own), counts, *parts, *vmem(centroids), *extra)


def sequence(n_mp):
    return [0, 1, 6, 2, 3, 7, 4, 5] if n_mp == 8 else list(range(n_mp))


def pieces_of(n_mp, feat):
    mid = feat // 2
    seq = sequence(n_mp)
    return [[(k, 0, feat)] if at < n_mp - 3 else [(k, 0, mid), (k, mid, mid)] for at, k in enumerate(seq)]


def own_groups(n_mp):
    return [(k, k + 1) for k in range(0, n_mp - 2, 2)] + [(n_mp - 2,)]


def on_square(data_rows, centroids, block_mask, lower_bound):
    feat = data_rows.shape[1]
    width = centroids.shape[0]
    block_count = data_rows.shape[0] // BLOCK
    n_mp = lax.axis_size("mp")
    n_dp = lax.axis_size("dp")
    own_width = width // n_dp
    half = own_width // 2
    my_mp = lax.axis_index("mp").astype(jnp.int32)
    my_dp = lax.axis_index("dp").astype(jnp.int32)
    sharpness = 4.0 / math.sqrt(feat)
    ids = jnp.stack([my_mp, my_dp])
    mask_t = block_mask.T

    seq = sequence(n_mp)
    last = seq[-1]
    cuts = {cut[0][0]: cut for cut in pieces_of(n_mp, feat)}
    early = [p for k in seq[2:5] for p in cuts[k]]
    late = cuts[0] + [p for k in seq[5:] for p in cuts[k]] + cuts[1]
    got = dict(zip(early, take_slots(ids, mask_t, data_rows, early, [])))
    *rest, codes = take_slots(ids, mask_t, data_rows, late, seq)
    got.update(zip(late, rest))
    for piece in early + late[1:]:
        got[piece] = swap(got[piece], "mp", n_mp, piece[0])

    side = {}
    for k in seq:
        for piece in cuts[k]:
            for bit in (1, 2):
                side[bit, piece] = swap(got[piece], "dp", n_dp, bit)

    cents, cent_norm = load_centroids(centroids, 2 * n_dp)

    n_rows = n_mp * BLOCK
    own = [
        jax.ShapeDtypeStruct((n_rows, feat), BF16),
        jax.ShapeDtypeStruct((own_width, n_rows), F32),
        jax.ShapeDtypeStruct((n_mp, 1, BLOCK), F32),
    ]
    sides = [jax.ShapeDtypeStruct((n_rows, feat), BF16)] * 2
    sides += [jax.ShapeDtypeStruct((3 * half, n_rows), F32)] * 2
    ahead = first_product(cents, got[cuts[last][0]], 1)
    for group in own_groups(n_mp):
        held = [p for at in group for p in cuts[seq[at]]]
        placed = [(seq.index(p[0]) - group[0], p[1], p[2]) for p in held]
        own = own_scores(
            ids, cents, cent_norm, [got[p] for p in held], placed, own, group[0] // len(group), len(group),
            n_dp, sharpness,
        )
    for i in range(n_mp // 2):
        held = cuts[seq[2 * i]] + cuts[seq[2 * i + 1]]
        placed = [(seq.index(p[0]) - 2 * i, p[1], p[2]) for p in held]
        pair = [[side[bit, p] for p in held] for bit in (1, 2)]
        for bit in (1, 2):
            sides[bit - 1 :: 2] = one_side_scores(
                ids, cents, cent_norm, pair[bit - 1], placed, sides[bit - 1 :: 2], i, 2, half, sharpness, bit
            )

    *own, note = last_scores(ids, cents, cent_norm, [got[p] for p in cuts[last]], ahead, codes, own, n_dp, sharpness)
    beside = swap(note, "mp", n_mp, 1)
    both = jnp.concatenate([note, beside])
    notes = [both]
    for k in range(2, n_mp, 2):
        notes.append(swap(both, "mp", n_mp, k))
    slot_norm, row_norm = combine(notes, seq, block_count)
    log_norm = row_norm.reshape(-1)
    side_norm = []
    for bit in (1, 2):
        side_norm.append(swap(slot_norm, "dp", n_dp, bit))

    tile = feat // 4
    spans = [(0, 2 * tile), (2 * tile, 2 * tile)]
    received = []
    for i, (first, columns) in enumerate(spans):
        sent = sent_sums(sides[:2], sides[2:], side_norm, half, first, columns, tile, i == 0)
        for_y, for_x = [v.astype(jnp.float16) for v in sent]
        pair = []
        for bit, message in ((1, for_x), (2, for_y)):
            pair.append(swap(message, "dp", n_dp, bit).astype(F32))
        received.append(pair)
    total, counts = own_sums(
        [own[0], sides[0], sides[1]], [own[1], sides[2], sides[3]], [slot_norm] + side_norm, own_width, tile
    )
    state = None
    for i, (first, columns) in enumerate(spans):
        state = update(ids, total, counts, received[i], cents, first, columns, state, i == len(spans) - 1, n_dp * n_mp)
    updated, movement, peak = state
    shard_peaks = lax.all_to_all(peak, ("dp", "mp"), split_axis=0, concat_axis=0, tiled=True)
    shard_peak = jnp.max(shard_peaks.reshape(n_dp, n_mp, LANES), axis=(0, 2))
    new_lower = lower_bound - shard_peak[:, None]
    return (updated, movement[:, 0], log_norm, new_lower)


def on_device(data_rows, centroids, block_mask, lower_bound):
    feat = data_rows.shape[1]
    width = centroids.shape[0]
    block_count = data_rows.shape[0] // BLOCK
    n_mp = lax.axis_size("mp")
    n_dp = lax.axis_size("dp")
    own_width = width // n_dp
    my_mp = lax.axis_index("mp")
    my_dp = lax.axis_index("dp")
    sharpness = 4.0 / math.sqrt(feat)

    labels = jnp.arange(1, block_count + 1, dtype=jnp.int32)
    codes = jnp.sum(block_mask * labels[None, :], axis=1)

    def outgoing(k):
        code = lax.dynamic_index_in_dim(codes, my_mp ^ k, 0, keepdims=False)
        start = jnp.maximum(code - 1, 0) * BLOCK
        return lax.dynamic_slice(data_rows, (start, 0), (BLOCK, feat))

    order = list(range(2, n_mp)) + [1]
    got = {0: outgoing(0)}
    for k in order:
        got[k] = swap(outgoing(k), "mp", n_mp, k)

    cent_norm = jnp.sum(jnp.square(centroids.astype(jnp.float32)), axis=1)

    scores, lses = {}, {}
    groups = [(k, k + 1) for k in range(0, n_mp, 2)]
    for group in groups:
        rows = jnp.concatenate([got[k] for k in group], axis=0)
        product = lax.dot_general(
            centroids, rows, (((1,), (1,)), ((), ())), preferred_element_type=jnp.float32
        )
        score = sharpness * (2.0 * product - cent_norm[:, None])
        top = jnp.max(score, axis=0)
        lse = top + jnp.log(jnp.sum(jnp.exp(score - top[None, :]), axis=0))
        scores[group] = score
        for i, k in enumerate(group):
            lses[k] = lse[i * BLOCK : (i + 1) * BLOCK]

    note = jnp.concatenate(
        [
            jnp.stack([lses[k] for k in range(n_mp)]),
            jnp.pad(codes.astype(jnp.float32), (0, BLOCK - n_mp))[None, :],
        ]
    )
    notes = lax.all_to_all(
        jnp.broadcast_to(note[None], (n_mp,) + note.shape), "mp", split_axis=0, concat_axis=0, tiled=True
    )
    shard_ids = jnp.arange(n_mp, dtype=jnp.int32)
    lse_of = notes[:, :n_mp, :]
    all_code = notes[:, n_mp, :n_mp].astype(jnp.int32)
    all_lse = lse_of[shard_ids[None, :], shard_ids[None, :] ^ shard_ids[:, None]]
    tops = jnp.where((all_code > 0)[:, :, None], all_lse, -1e30)

    def normalizer(same, lse):
        kept = jnp.where(same[:, :, None], lse, -1e30)
        peak = jnp.maximum(jnp.max(kept, axis=1), 0.0)
        mass = jnp.sum(jnp.exp(kept - peak[:, None, :]), axis=1)
        return peak + jnp.log(jnp.exp(-peak) + mass)

    my_lse = lax.dynamic_index_in_dim(tops, my_mp, 0, keepdims=False)
    row_norm = normalizer(codes[None, :] == labels[:, None], jnp.broadcast_to(my_lse[None], (block_count,) + my_lse.shape))
    log_norm = row_norm.reshape(-1)

    slot_code = lax.dynamic_index_in_dim(all_code, my_mp, 1, keepdims=False)
    slot_norm = normalizer((all_code == slot_code[:, None]) & (all_code > 0), tops)

    weights, counts = [], 0.0
    for group in groups:
        src = [my_mp ^ k for k in group]
        norm = jnp.concatenate([slot_norm[m] for m in src])
        valid = jnp.concatenate([jnp.broadcast_to(slot_code[m] > 0, (BLOCK,)) for m in src])
        weight = jnp.where(valid[None, :], jnp.exp(scores[group] - norm[None, :]), 0.0)
        counts = counts + jnp.sum(weight, axis=1)
        weights.append(weight.astype(jnp.bfloat16))
    weight_half = jnp.concatenate(weights, axis=1)
    rows = jnp.concatenate([got[k] for k in range(n_mp)], axis=0)

    def quarter(j):
        return (my_dp ^ j) * own_width

    def partial(j, half):
        w = lax.dynamic_slice(weight_half, (quarter(j), 0), (own_width, weight_half.shape[1]))
        x = lax.slice_in_dim(rows, half * (feat // 2), (half + 1) * (feat // 2), axis=1)
        return lax.dot_general(w, x, (((1,), (0,)), ((), ())), preferred_element_type=jnp.float32)

    count_of = {0: counts}
    for j in range(1, n_dp):
        count_of[j] = swap(counts, "dp", n_dp, j)

    def sub(vec, j):
        return lax.dynamic_slice(vec, (quarter(j),), (own_width,))

    def scale(members, j):
        total = sum(sub(count_of[i], j) for i in members)
        return jnp.maximum(total, 2.0**-20)[:, None] * 2.0**-10

    bits = [1 << b for b in range(n_dp.bit_length() - 1)]
    plan = [bits, bits[::-1]]
    current = [{}, {}]
    for j in reversed(range(n_dp)):
        for half in range(2):
            jj = j if half == 0 or n_dp != 4 else {3: 3, 1: 2, 2: 1, 0: 0}[j]
            current[half][jj] = None
    todo = [[j for j in reversed(range(n_dp))] for _ in range(2)]
    for half in range(2):
        for j in todo[half]:
            current[half][j] = partial(j, half)
    members = [{0}, {0}]
    for step in range(len(bits)):
        for half in range(2):
            bit = plan[half][step]
            cur = current[half]
            mine = members[half]
            theirs = {i ^ bit for i in mine}
            kept = {}
            for j in sorted(cur, reverse=True):
                if not j & bit:
                    continue
                sent = (cur[j] / scale(mine, j)).astype(jnp.float16)
                back = swap(sent, "dp", n_dp, bit)
                kept[j ^ bit] = cur[j ^ bit] + back.astype(jnp.float32) * scale(theirs, j ^ bit)
            current[half] = kept
            members[half] = mine | theirs
    part_sums = jnp.concatenate([current[0][0], current[1][0]], axis=1)
    part_counts = sum(sub(count_of[j], 0) for j in range(n_dp))

    old_cents = lax.dynamic_slice_in_dim(centroids, my_dp * own_width, own_width, 0).astype(jnp.float32)
    updated = (part_sums + old_cents) / (part_counts[:, None] + 1.0)
    movement = jnp.sqrt(jnp.sum(jnp.square(updated - old_cents), axis=1) + 1.0)
    peak = jnp.broadcast_to(jnp.max(movement), (n_dp * n_mp, 1))
    shard_peaks = lax.all_to_all(peak, ("dp", "mp"), split_axis=0, concat_axis=0, tiled=True)
    shard_peak = jnp.max(shard_peaks.reshape(n_dp, n_mp), axis=0)
    new_lower = lower_bound - shard_peak[:, None]
    return (updated, movement, log_norm, new_lower)


def solution(mesh):
    placed = (P(("dp", "mp"), None), P("mp", None), P(None, ("dp", "mp")), P(None, ("dp", "mp")))
    square = mesh.shape["dp"] == 4

    def body(*args):
        return on_square(*args) if square else on_device(*args)

    return jax.shard_map(
        body,
        mesh=mesh,
        in_specs=placed,
        out_specs=(P(("mp", "dp"), None), P(("mp", "dp")), P(("dp", "mp")), P(None, ("dp", "mp"))),
        check_vma=False,
    )
```
